128 devices in a mesh: var: 16 (over x, y), samp: 8 (over z, core).
Axes of the slice: x: 4, y: 4, z: 4, core: 2. Of those that a mesh axis runs over, the one named last changes fastest.
Arguments:
- dosage: int32 [24576, 8192], P('samp', 'var'), may hold values from 0 to 2, as said below
- phenotype: float32 [24576], P('samp'), may hold values from -6 to 6
- perm_index: int32 [1024, 24576], P('var', 'samp'), may hold values from 0 to 24575, each once within a row
- seg_lengths: int32 [128], replicated, may hold values from 1 to 128, 8192 in all
Outputs:
- zscore: float32 [1024, 8192], P('samp', 'var')
- thresholds: float32 [1024, 128], P('samp')
The draws below stay inside these ranges and needn't reach their ends.
Inputs may be any that keep to these rules, and one draw needn't show every extreme that they name: `dosage`: each entry is an allele count. `perm_index`: each row is a permutation of the 24576 sample numbers. `seg_lengths`: the lengths sum to 8192, one of them equals 128.
All inputs are finite; a program needn't handle non-finite values.
Results may differ from the reference program's by a relative error of at most 0.0039.
Values may be sent and summed in bfloat16 or wider, within the bound.
No kernel may reach another device: no remote copies, remote signals or barrier semaphores. Data moves between devices by JAX's collectives and lax.ppermute only.
A program may use at most 64 MiB of HBM per device.

```python
import math
import jax
import jax.numpy as jnp
import numpy as np
from jax import lax

PERMS = 1024
SEGS = 128
SAMPLES = 24576
V = 8192
SEG_MOST = 128


def draw_dosage(key, part):
    rate_key, one_key, two_key = jax.random.split(jax.random.fold_in(key, 17), 3)
    allele_rate = jax.random.randint(rate_key, (1, V), 20, 300)
    cohort_rise = 1000 + 2000 * jnp.arange(SAMPLES, dtype=jnp.int32) // SAMPLES
    level = allele_rate * cohort_rise[:, None] // 1000
    allele_one = jax.random.randint(one_key, (SAMPLES, V), 0, 1000) < level
    allele_two = jax.random.randint(two_key, (SAMPLES, V), 0, 1000) < level
    return allele_one.astype(jnp.int32) + allele_two.astype(jnp.int32)


def steps_of(rng, dims, cuts, least, top_value):
    def one(axis_at, blocks):
        draws = jax.random.uniform(jax.random.fold_in(jax.random.fold_in(rng, 6), axis_at), (blocks,), jnp.float32, least / len(cuts), top_value / len(cuts))
        return jnp.repeat(jnp.exp(draws), dims[axis_at] // blocks).reshape((-1,) + (1,) * (len(dims) - axis_at - 1))

    level = one(*cuts[0])
    for cut in cuts[1:]:
        level = level * one(*cut)
    return level


def split_up(number_of, total, bound, slope):
    portions = [(1 << 20) // math.isqrt(rank ** slope) + 1 for rank in range(2, number_of + 1)]
    surplus, holding = total - bound - (number_of - 1), [1] * (number_of - 1)
    while surplus > 0:
        movable = [i for i in range(number_of - 1) if holding[i] < bound]
        pool, budget = sum([portions[i] for i in movable]), surplus
        for i in movable:
            extra = min(bound - holding[i], max(1, budget * portions[i] // pool), surplus)
            holding[i] = holding[i] + extra
            surplus = surplus - extra
    return np.array([bound] + holding)


def uneven_parts(key, count, total, most, lean):
    if count == 2:
        one = jax.random.randint(key, (), max(1, total - most), min(most, total - 1) + 1)
        return jnp.stack([one, total - one])
    tallies = jnp.asarray(split_up(count, total, most, lean), jnp.int32)
    twos = (count - 1) // 2
    source_of, taker = tallies[1:1 + 2 * twos:2], tallies[2:2 + 2 * twos:2]
    room = jnp.minimum(source_of - 1, most - taker)
    moved = jax.random.randint(jax.random.fold_in(key, 1), (twos,), 0, 1 << 20) % (room + 1)
    tallies = tallies.at[1:1 + 2 * twos:2].set(source_of - moved).at[2:2 + 2 * twos:2].set(taker + moved)
    return tallies[jax.random.permutation(jax.random.fold_in(key, 2), count)]


def gaussian(rng, extent, spread, most, shards=(), kind=jnp.bfloat16):
    gain = steps_of(rng, extent, shards, -0.22, 0.18) if shards else 1.0
    entries = jax.random.normal(rng, extent, jnp.float32) * spread * gain
    return jnp.minimum(jnp.maximum(entries, -most), most).astype(kind)


def setup_inputs(seed: int = 0) -> dict:
    splits = jax.random.split(jax.random.key(seed), 5)
    return {
        "dosage": draw_dosage(jax.random.fold_in(splits[4], 71), 0),
        "phenotype": gaussian(splits[1], (SAMPLES,), 1.0, 6.0, ((0, 8),), jnp.float32),
        "perm_index": jax.vmap(lambda own: jax.random.permutation(own, SAMPLES))(jax.random.split(splits[2], PERMS)).reshape((PERMS, SAMPLES)).astype(jnp.int32),
        "seg_lengths": uneven_parts(splits[3], SEGS, V, SEG_MOST, 2).astype(jnp.int32),
    }


epsilon = 1e-05

def reference(dosage, phenotype, perm_index, seg_lengths):
    count_all = phenotype.shape[0]
    centered = phenotype - jnp.mean(phenotype)
    pheno_var = jnp.mean(centered * centered)
    rounded = centered.astype(jnp.bfloat16)
    allele_sum = lax.optimization_barrier(jnp.sum(dosage, axis=0)).astype(jnp.float32)
    allele_sq = lax.optimization_barrier(jnp.sum(dosage * dosage, axis=0)).astype(jnp.float32)
    allele_var = allele_sq / count_all - (allele_sum / count_all) ** 2
    dosage_bf = dosage.astype(jnp.bfloat16)
    block_rows = min(128, PERMS)
    grouped = perm_index.reshape(PERMS // block_rows, block_rows, count_all)

    def score_block(index_rows):
        permuted = jnp.take(rounded, index_rows, axis=0)
        return jnp.dot(permuted, dosage_bf, preferred_element_type=jnp.float32)
    score = lax.map(score_block, grouped).reshape(PERMS, dosage.shape[1])
    divisor = jnp.sqrt(count_all * (pheno_var + epsilon) * (allele_var + epsilon))
    zscore = score / divisor[None, :]
    prefix = lax.cummax(jnp.abs(zscore), axis=1)
    segment_end = (jnp.cumsum(seg_lengths) - 1).astype(jnp.int32)
    thresholds = jnp.take(prefix, segment_end, axis=1)
    return (zscore, thresholds)
```

```python
import jax
import jax.numpy as jnp
from jax import lax
from jax.experimental import pallas as pl
from jax.experimental.pallas import tpu as pltpu
from jax.sharding import Mesh, PartitionSpec as P


EPSILON = 1e-05
RING = 4
AXES = ("x", "y", "z", "c")
CHUNKS = 2
LOW = 128
PLACES = [
    (x, y, z, c) for x in range(RING) for y in range(RING) for z in range(RING) for c in range(2)
]


def at(x, y, z, c):
    return (((x % RING) * RING + y % RING) * RING + z % RING) * 2 + c


def shift(value, target):
    return lax.ppermute(value, AXES, [(at(*d), at(*target(*d))) for d in PLACES])


def along(value, axis, step):
    return lax.ppermute(value, axis, [(i, (i + step) % RING) for i in range(RING)])


def other_core(value):
    return lax.ppermute(value, "c", [(0, 1), (1, 0)])


def make_table(rounded, rows):
    size = jnp.abs(rounded)
    most = jnp.maximum(jnp.max(size), 1e-30)
    code = jnp.round(jnp.sqrt(jnp.sqrt(size / most)) * 32767.0).astype(jnp.int32)
    code = jnp.where(rounded < 0, -code, code)
    half = rows // 2
    table = lax.shift_left(code[half:], 16) + (code[:half] & 0xFFFF)
    scale = jnp.sqrt(jnp.sqrt(most)) / 32767.0
    return table, scale.reshape(1, 1)


def lookup_kernel(index_ref, table_ref, scale_ref, out_ref):
    rows, width = index_ref.shape
    half = table_ref.shape[0]
    scale = scale_ref[0, 0]
    span = 2 * LOW

    def step(j, _):
        for part in range(2):
            base = pl.multiple_of(j * span + part * LOW, LOW)
            found = []
            for i in range(0, rows, 8):
                index = index_ref[pl.ds(i, 8), pl.ds(base, LOW)]
                lane = index & (LOW - 1)
                row = lax.shift_right_logical(index, 7)
                upper = row >= half
                row = jnp.where(upper, row - half, row)
                word = jnp.zeros((8, LOW), jnp.int32)
                for r in range(half):
                    source = jnp.broadcast_to(table_ref[r : r + 1, :], (8, LOW))
                    taken = jnp.take_along_axis(source, lane, axis=1, mode="promise_in_bounds")
                    word = jnp.where(row == r, taken, word)
                code = lax.shift_right_arithmetic(
                    jnp.where(upper, word, lax.shift_left(word, 16)), 16
                )
                root = code.astype(jnp.float32) * scale
                root = root * root
                root = root * root
                found.append(jnp.where(code < 0, -root, root))
            out_ref[:, pl.ds(base, LOW)] = jnp.concatenate(found, axis=0).astype(jnp.bfloat16)
        return 0

    lax.fori_loop(0, width // span, step, 0)


def lookup(index, table, scale):
    vmem = pl.BlockSpec(memory_space=pltpu.VMEM)
    return pl.pallas_call(
        lookup_kernel,
        out_shape=jax.ShapeDtypeStruct(index.shape, jnp.bfloat16),
        in_specs=[vmem, vmem, pl.BlockSpec(memory_space=pltpu.SMEM)],
        out_specs=vmem,
    )(index, table, scale)


def ring_gather(value, first, turn):
    def line(step):
        def target(x, y, z, c):
            if (c == 0) == first:
                return (x + step, y, z, c)
            return (x, y + step, z, c)

        return target

    def onward(x, y, z, c):
        step = 1 if c == turn else -1
        if (c == 0) == first:
            return (x + step, y, z, c)
        return (x, y + step, z, c)

    from_before = shift(value, line(1))
    from_after = shift(value, line(-1))
    passed = jnp.where(lax.axis_index("c") == turn, from_before, from_after)
    return [value, from_before, from_after, shift(passed, onward)]


PIECE_OF = (0, 2, 3, 1)


def product_kernel(dest_ref, a0, a1, a2, a3, dosage_ref, out_ref):
    rows = a0.shape[1]
    for u, a in enumerate((a0, a1, a2, a3)):
        block = a[...].reshape(RING * rows, a.shape[2])
        part = jnp.dot(block, dosage_ref[...], preferred_element_type=jnp.float32)
        for t in range(RING):
            start = pl.multiple_of(dest_ref[u * RING + t] * rows, rows)
            out_ref[pl.ds(start, rows), :] = part[t * rows : (t + 1) * rows]


def product(dest, pieces, dosage):
    vmem = pl.BlockSpec(memory_space=pltpu.VMEM)
    rows = pieces[0].shape[1] * RING * RING
    return pl.pallas_call(
        product_kernel,
        out_shape=jax.ShapeDtypeStruct((rows, dosage.shape[1]), jnp.float32),
        in_specs=[pl.BlockSpec(memory_space=pltpu.SMEM)] + [vmem] * 5,
        out_specs=vmem,
    )(dest, *pieces, dosage)


def destinations():
    x, y, z, c = (lax.axis_index(a) for a in AXES)
    offset = jnp.array([0, 3, 1, 2], jnp.int32)
    u, t = offset[:, None], offset[None, :]
    dx = jnp.where(c == 0, t, u)
    dy = jnp.where(c == 0, u, t)
    px, py = (x + dx) % RING, (y + dy) % RING
    away = jnp.where(py // 2 == c, 0, 1)
    return (away * 8 + ((px - z) % RING) * 2 + py % 2).reshape(-1).astype(jnp.int32)


def final_kernel(s0, s1, s2, s3, inverse_ref, end_ref, z_ref, most_ref):
    rows, width = z_ref.shape
    z = (s0[...] + s1[...] + s2[...] + s3[...]) * inverse_ref[...]
    z_ref[...] = z
    ends = end_ref[...]
    lanes = lax.broadcasted_iota(jnp.int32, (8, LOW), 1)
    inside = ends >= 0
    clipped = jnp.clip(ends, 0, width - 1)
    lane = jnp.broadcast_to(clipped % LOW, (8, LOW))
    group = jnp.broadcast_to(clipped // LOW, (8, LOW))
    ok = jnp.broadcast_to(inside, (8, LOW))
    for i in range(0, rows, 8):
        before = jnp.zeros((8, 1), jnp.float32)
        chosen = jnp.zeros((8, LOW), jnp.float32)
        for g in range(width // LOW):
            part = jnp.abs(z[i : i + 8, g * LOW : (g + 1) * LOW])
            whole = jnp.max(part, axis=1, keepdims=True)
            step = 1
            while step < LOW:
                moved = pltpu.roll(part, step, 1)
                part = jnp.maximum(part, jnp.where(lanes >= step, moved, 0.0))
                step *= 2
            part = jnp.maximum(part, before)
            taken = jnp.take_along_axis(part, lane, axis=1, mode="promise_in_bounds")
            chosen = jnp.where(group == g, taken, chosen)
            before = jnp.maximum(before, whole)
        most_ref[pl.ds(i, 8), :] = jnp.where(ok, chosen, 0.0)


def final(parts, inverse, ends):
    vmem = pl.BlockSpec(memory_space=pltpu.VMEM)
    rows, width = parts[0].shape
    return pl.pallas_call(
        final_kernel,
        out_shape=(
            jax.ShapeDtypeStruct((rows, width), jnp.float32),
            jax.ShapeDtypeStruct((rows, ends.shape[1]), jnp.float32),
        ),
        in_specs=[vmem] * 6,
        out_specs=(vmem, vmem),
    )(*parts, inverse, ends)


def largest(value, axis):
    got = [along(value, axis, k) for k in (1, 3, 2)]
    return jnp.maximum(jnp.maximum(value, got[0]), jnp.maximum(got[1], got[2]))


def per_device(dosage, phenotype, perm_index, seg_lengths):
    samples, width = dosage.shape
    x, y, z, c = (lax.axis_index(a) for a in AXES)
    dosage_bf = dosage.astype(jnp.bfloat16)
    allele_sum = jnp.sum(dosage, axis=0).astype(jnp.float32)
    allele_sq = jnp.sum(dosage * dosage, axis=0).astype(jnp.float32)
    own = jnp.concatenate([phenotype, allele_sum, allele_sq]).reshape(-1, LOW)

    other = other_core(own)
    pair = jnp.where(c == 0, jnp.stack([own, other]), jnp.stack([other, own]))
    from_1, from_3, from_2 = (along(pair, "z", k) for k in (1, 3, 2))
    by_offset = jnp.stack([pair, from_3, from_2, from_1])
    twice = jnp.concatenate([by_offset, by_offset])
    ordered = lax.dynamic_slice_in_dim(twice, (RING - z) % RING, RING, 0)
    blocks = ordered.reshape(2 * RING, -1, LOW)
    depth = samples // LOW
    traits = blocks[:, :depth].reshape(-1, LOW)
    totals = blocks[:, depth:].sum(axis=0).reshape(2, width)

    count_all = traits.size
    centered = traits - jnp.mean(traits)
    pheno_var = jnp.mean(centered * centered)
    rounded = centered.astype(jnp.bfloat16).astype(jnp.float32)
    table, scale = make_table(rounded, traits.shape[0])

    allele_var = totals[1] / count_all - (totals[0] / count_all) ** 2
    inverse = 1.0 / jnp.sqrt(count_all * (pheno_var + EPSILON) * (allele_var + EPSILON))
    inverse = inverse[None, :]
    ends = (jnp.cumsum(seg_lengths) - 1 - (x * RING + y) * width)[None, :].astype(jnp.int32)
    dest = destinations()

    perms = perm_index.shape[0]
    rows = perms // CHUNKS
    scores, picks = [], []
    for k in range(CHUNKS):
        permuted = lookup(perm_index[k * rows : (k + 1) * rows], table, scale)
        turn = k % 2
        near = jnp.stack(ring_gather(permuted, True, turn))
        pieces = ring_gather(near, False, 1 - turn)
        partial = product(dest, pieces, dosage_bf)
        half = partial.shape[0] // 2
        summed = partial[:half] + other_core(partial[half:])
        summed = summed.reshape(RING, half // RING, width)
        parts = [summed[0]] + [along(summed[j], "z", j) for j in (1, 2, 3)]
        score, pick = final(parts, inverse, ends)
        scores.append(score.reshape(2, rows, width))
        pick = largest(largest(pick, "x"), "y")
        picks.append(pick.reshape(2, rows, -1))
    zscore = jnp.concatenate(scores, axis=1).reshape(2 * perms, width)
    thresholds = jnp.concatenate(picks, axis=1).reshape(2 * perms, -1)
    return (zscore, thresholds)


def solution(mesh):
    fine = Mesh(mesh.devices.reshape(RING, RING, RING, 2), AXES)
    var, samp = ("x", "y"), ("z", "c")
    return jax.shard_map(
        per_device,
        mesh=fine,
        in_specs=(P(samp, var), P(samp), P(var, samp), P()),
        out_specs=(P(samp, var), P(samp, None)),
        check_vma=False,
    )
```

```python
import jax
import jax.numpy as jnp
from jax import lax
from jax.experimental import pallas as pl
from jax.experimental.pallas import tpu as pltpu
from jax.sharding import Mesh, PartitionSpec as P


EPSILON = 1e-05
RING = 4
AXES = ("x", "y", "z", "c")
CHUNKS = 2
LOW = 128
AT_ONCE = 24
PLACES = [
    (x, y, z, c) for x in range(RING) for y in range(RING) for z in range(RING) for c in range(2)
]
VMEM = pl.BlockSpec(memory_space=pltpu.VMEM)
SMEM = pl.BlockSpec(memory_space=pltpu.SMEM)


def at(x, y, z, c):
    return (((x % RING) * RING + y % RING) * RING + z % RING) * 2 + c


def shift(value, target):
    return lax.ppermute(value, AXES, [(at(*d), at(*target(*d))) for d in PLACES])


def along(value, axis, step):
    return lax.ppermute(value, axis, [(i, (i + step) % RING) for i in range(RING)])


def other_core(value):
    return lax.ppermute(value, "c", [(0, 1), (1, 0)])


def out_of(shape, dtype):
    return jax.ShapeDtypeStruct(shape, dtype)


def dosage_kernel(dosage_ref, out_ref, totals_ref, acc_ref):
    @pl.when(pl.program_id(0) == 0)
    def _():
        acc_ref[...] = jnp.zeros_like(acc_ref)

    d = dosage_ref[...]
    out_ref[...] = d.astype(jnp.bfloat16)
    groups = d.reshape(d.shape[0] // 8, 8, d.shape[1])
    acc_ref[0:8] += jnp.sum(groups, axis=0)
    acc_ref[8:16] += jnp.sum(groups * groups, axis=0)

    @pl.when(pl.program_id(0) == pl.num_programs(0) - 1)
    def _():
        totals_ref[...] = acc_ref[...].astype(jnp.float32)


def convert_dosage(dosage):
    samples, width = dosage.shape
    block = 512
    return pl.pallas_call(
        dosage_kernel,
        grid=(samples // block,),
        out_shape=(out_of(dosage.shape, jnp.bfloat16), out_of((16, width), jnp.float32)),
        in_specs=[pl.BlockSpec((block, width), lambda i: (i, 0))],
        out_specs=(
            pl.BlockSpec((block, width), lambda i: (i, 0)),
            pl.BlockSpec((16, width), lambda i: (0, 0)),
        ),
        scratch_shapes=[pltpu.VMEM((16, width), jnp.int32)],
    )(dosage)


def table_kernel(place_ref, p0, p1, p2, p3, table_ref, scale_ref, var_ref, code_ref):
    z, c = place_ref[0], place_ref[1]
    refs = (p0, p1, p2, p3)
    depth = p0.shape[1]
    count = len(refs) * p0.size
    mean = sum(jnp.sum(r[...]) for r in refs) / count
    var_ref[0, 0] = sum(jnp.sum((r[...] - mean) ** 2) for r in refs) / count
    rounded = [(r[...] - mean).astype(jnp.bfloat16).astype(jnp.float32) for r in refs]
    most = jnp.float32(1e-30)
    for r in rounded:
        most = jnp.maximum(most, jnp.max(jnp.abs(r)))
    most = jnp.full((1, LOW), most, jnp.float32)
    for k, r in enumerate(rounded):
        code = jnp.round(jnp.sqrt(jnp.sqrt(jnp.abs(r) / most)) * 32767.0).astype(jnp.int32)
        code = jnp.where(r < 0, -code, code)
        for j in range(2):
            core = c if j == 0 else 1 - c
            start = (((z + RING - k) % RING) * 2 + core) * depth
            code_ref[pl.ds(pl.multiple_of(start, 8), depth), :] = code[j]
    half = table_ref.shape[0]
    table_ref[...] = lax.shift_left(code_ref[half:, :], 16) + (code_ref[:half, :] & 0xFFFF)
    scale_ref[...] = jnp.sqrt(jnp.sqrt(most)) / 32767.0


def make_table(place, pairs):
    rows = len(pairs) * pairs[0].shape[0] * pairs[0].shape[1]
    return pl.pallas_call(
        table_kernel,
        out_shape=(
            out_of((rows // 2, LOW), jnp.int32),
            out_of((1, LOW), jnp.float32),
            out_of((1, 1), jnp.float32),
        ),
        in_specs=[SMEM] + [VMEM] * 4,
        out_specs=(VMEM, VMEM, SMEM),
        scratch_shapes=[pltpu.VMEM((rows, LOW), jnp.int32)],
    )(place, *pairs)


def lookup_kernel(index_ref, table_ref, scale_ref, out_ref):
    rows, width = index_ref.shape
    half = table_ref.shape[0]
    parts = AT_ONCE // (rows // 8)
    span = parts * LOW
    scale = jnp.broadcast_to(scale_ref[...], (8, LOW))

    def step(j, _):
        for part in range(parts):
            base = pl.multiple_of(j * span + part * LOW, LOW)
            found = []
            for i in range(0, rows, 8):
                index = index_ref[pl.ds(i, 8), pl.ds(base, LOW)]
                lane = index & (LOW - 1)
                row = lax.shift_right_logical(index, 7)
                upper = row >= half
                row = jnp.where(upper, row - half, row)
                word = jnp.zeros((8, LOW), jnp.int32)
                for r in range(half):
                    source = jnp.broadcast_to(table_ref[r : r + 1, :], (8, LOW))
                    taken = jnp.take_along_axis(source, lane, axis=1, mode="promise_in_bounds")
                    word = jnp.where(row == r, taken, word)
                code = lax.shift_right_arithmetic(
                    jnp.where(upper, word, lax.shift_left(word, 16)), 16
                )
                root = code.astype(jnp.float32) * scale
                root = root * root
                root = root * root
                found.append(jnp.where(code < 0, -root, root))
            out_ref[:, pl.ds(base, LOW)] = jnp.concatenate(found, axis=0).astype(jnp.bfloat16)
        return 0

    lax.fori_loop(0, width // span, step, 0)


def lookup(index, table, scale):
    return pl.pallas_call(
        lookup_kernel,
        out_shape=out_of(index.shape, jnp.bfloat16),
        in_specs=[VMEM] * 3,
        out_specs=VMEM,
    )(index, table, scale)


def ring_gather(value, first, turn):
    def line(sign):
        def target(x, y, z, c):
            step = sign if c == turn else -sign
            if (c == 0) == first:
                return (x + step, y, z, c)
            return (x, y + step, z, c)

        return target

    behind = shift(value, line(1))
    ahead = shift(value, line(-1))
    return [value, behind, ahead, shift(behind, line(1))]


def offsets(turn):
    step = jnp.where(lax.axis_index("c") == turn, 1, -1)
    return jnp.stack([0 * step, -step, step, 0 * step + 2])


def stack_kernel(a0, a1, a2, a3, out_ref):
    for k, a in enumerate((a0, a1, a2, a3)):
        out_ref[k] = a[...]


def stacked(pieces):
    return pl.pallas_call(
        stack_kernel,
        out_shape=out_of((len(pieces), *pieces[0].shape), pieces[0].dtype),
        in_specs=[VMEM] * 4,
        out_specs=VMEM,
    )(*pieces)


def product_kernel(dest_ref, a0, a1, a2, a3, dosage_ref, totals_ref, keep_ref, send_ref, lhs_ref):
    rows = a0.shape[1]
    extra = keep_ref.shape[1] - 2 * rows
    for u, a in enumerate((a0, a1, a2, a3)):
        for t in range(RING):
            start = pl.multiple_of(dest_ref[u * RING + t] * rows, rows)
            lhs_ref[pl.ds(start, rows), :] = a[t]
    part = jnp.dot(lhs_ref[...], dosage_ref[...], preferred_element_type=jnp.float32)
    for h, ref in enumerate((keep_ref, send_ref)):
        for k in range(RING):
            start = (h * RING + k) * 2 * rows
            ref[k, : 2 * rows, :] = part[start : start + 2 * rows]
            if extra:
                ref[k, 2 * rows :, :] = totals_ref[...]


def product(dest, pieces, dosage, totals, with_totals):
    rows = pieces[0].shape[1]
    shape = (RING, 2 * rows + (totals.shape[0] if with_totals else 0), dosage.shape[1])
    return pl.pallas_call(
        product_kernel,
        out_shape=(out_of(shape, jnp.float32), out_of(shape, jnp.float32)),
        in_specs=[SMEM] + [VMEM] * 6,
        out_specs=(VMEM, VMEM),
        scratch_shapes=[pltpu.VMEM((rows * RING * RING, dosage.shape[0]), jnp.bfloat16)],
    )(dest, *pieces, dosage, totals)


def add_kernel(a_ref, b_ref, o0, o1, o2, o3):
    for k, o in enumerate((o0, o1, o2, o3)):
        o[...] = a_ref[k] + b_ref[k]


def core_sum(keep, got):
    one = out_of(keep.shape[1:], jnp.float32)
    return pl.pallas_call(
        add_kernel, out_shape=(one,) * 4, in_specs=[VMEM] * 2, out_specs=(VMEM,) * 4
    )(keep, got)


def destinations(turn_near, turn_far):
    x, y, z, c = (lax.axis_index(a) for a in AXES)
    step = jnp.where(c == 0, 1, -1)
    u, t = offsets(turn_far)[:, None], offsets(turn_near)[None, :]
    px = (x + RING + jnp.where(c == 0, t, u)) % RING
    py = (y + RING + jnp.where(c == 0, u, t)) % RING
    away = jnp.where(py // 2 == c, 0, 1)
    step = jnp.where(away == 0, step, -step)
    owner = (step * (px - z) + 2 * RING) % RING
    return (away * 8 + owner * 2 + py % 2).reshape(-1).astype(jnp.int32)


def z_line(sign):
    def target(x, y, z, c):
        return (x, y, z + (sign if c == 0 else -sign), c)

    return target


def owner_parts(summed):
    own, ahead, opposite, behind = summed
    passing = shift(opposite, z_line(1))
    from_ahead = shift(behind, z_line(-1))
    from_behind = shift(ahead + passing, z_line(1))
    return [own, from_behind, from_ahead]


def final_kernel(var_ref, end_ref, a0, a1, a2, b0, b1, b2, z_ref, most_ref, *, count):
    rows = b0.shape[0] // 2
    width = z_ref.shape[1]
    totals = a0[2 * rows :, :] + a1[2 * rows :, :] + a2[2 * rows :, :]
    allele_sum = jnp.sum(totals[0:8], axis=0, keepdims=True)
    allele_sq = jnp.sum(totals[8:16], axis=0, keepdims=True)
    allele_var = allele_sq / count - (allele_sum / count) ** 2
    inverse = 1.0 / jnp.sqrt(count * (var_ref[0, 0] + EPSILON) * (allele_var + EPSILON))
    ends = end_ref[...]
    clipped = jnp.clip(ends, 0, width - 1)
    for chunk, (p, q, r) in enumerate(((a0, a1, a2), (b0, b1, b2))):
        for h in range(2):
            take = slice(h * rows, (h + 1) * rows)
            z = (p[take, :] + q[take, :] + r[take, :]) * inverse
            start = (h * CHUNKS + chunk) * rows
            z_ref[pl.ds(start, rows), :] = z
            lanes = lax.broadcasted_iota(jnp.int32, (rows, LOW), 1)
            lane = jnp.broadcast_to(clipped % LOW, (rows, LOW))
            group = jnp.broadcast_to(clipped // LOW, (rows, LOW))
            before = jnp.zeros((rows, 1), jnp.float32)
            chosen = jnp.zeros((rows, LOW), jnp.float32)
            for g in range(width // LOW):
                part = jnp.abs(z[:, g * LOW : (g + 1) * LOW])
                whole = jnp.max(part, axis=1, keepdims=True)
                step = 1
                while step < LOW:
                    moved = pltpu.roll(part, step, 1)
                    part = jnp.maximum(part, jnp.where(lanes >= step, moved, 0.0))
                    step *= 2
                part = jnp.maximum(part, before)
                taken = jnp.take_along_axis(part, lane, axis=1, mode="promise_in_bounds")
                chosen = jnp.where(group == g, taken, chosen)
                before = jnp.maximum(before, whole)
            inside = jnp.broadcast_to(ends >= 0, (rows, LOW))
            most_ref[pl.ds(start, rows), :] = jnp.where(inside, chosen, 0.0)


def final(pheno_var, ends, first, second, count):
    rows, width = second[0].shape
    return pl.pallas_call(
        lambda *refs: final_kernel(*refs, count=count),
        out_shape=(
            out_of((CHUNKS * rows, width), jnp.float32),
            out_of((CHUNKS * rows, ends.shape[1]), jnp.float32),
        ),
        in_specs=[SMEM] + [VMEM] * 7,
        out_specs=(VMEM, VMEM),
    )(pheno_var, ends, *first, *second)


def largest(value, axis):
    value = jnp.maximum(value, along(value, axis, 1))
    return jnp.maximum(value, along(value, axis, 2))


def per_device(dosage, phenotype, perm_index, seg_lengths):
    samples, width = dosage.shape
    x, y, z, c = (lax.axis_index(a) for a in AXES)
    own = phenotype.reshape(-1, LOW)
    pair = jnp.stack([own, other_core(own)])
    pairs = [pair] + [along(pair, "z", k) for k in (1, 2, 3)]
    dosage_bf, totals = convert_dosage(dosage)
    place = jnp.stack([z, c]).astype(jnp.int32)
    table, scale, pheno_var = make_table(place, pairs)
    ends = (jnp.cumsum(seg_lengths) - 1 - (x * RING + y) * width)[None, :].astype(jnp.int32)

    perms = perm_index.shape[0]
    rows = perms // CHUNKS
    parts = []
    for k in range(CHUNKS):
        permuted = lookup(perm_index[k * rows : (k + 1) * rows], table, scale)
        turn = k % 2
        near = stacked(ring_gather(permuted, True, turn))
        pieces = ring_gather(near, False, 1 - turn)
        dest = destinations(turn, 1 - turn)
        keep, send = product(dest, pieces, dosage_bf, totals, k == 0)
        parts.append(owner_parts(core_sum(keep, other_core(send))))
    count = float(samples * lax.axis_size("z") * lax.axis_size("c"))
    zscore, most = final(pheno_var, ends, parts[0], parts[1], count)
    return (zscore, largest(largest(most, "x"), "y"))


def solution(mesh):
    fine = Mesh(mesh.devices.reshape(RING, RING, RING, 2), AXES)
    var, samp = ("x", "y"), ("z", "c")
    return jax.shard_map(
        per_device,
        mesh=fine,
        in_specs=(P(samp, var), P(samp), P(var, samp), P()),
        out_specs=(P(samp, var), P(samp, None)),
        check_vma=False,
    )
```

```python
import jax
import jax.numpy as jnp
from jax import lax
from jax.experimental import pallas as pl
from jax.experimental.pallas import tpu as pltpu
from jax.sharding import Mesh, PartitionSpec as P


EPSILON = 1e-05
RING = 4
AXES = ("x", "y", "z", "c")
CHUNKS = 2
LOW = 128
AT_ONCE = 24
PLACES = [
    (x, y, z, c) for x in range(RING) for y in range(RING) for z in range(RING) for c in range(2)
]
VMEM = pl.BlockSpec(memory_space=pltpu.VMEM)
SMEM = pl.BlockSpec(memory_space=pltpu.SMEM)


def at(x, y, z, c):
    return (((x % RING) * RING + y % RING) * RING + z % RING) * 2 + c


def shift(value, target):
    return lax.ppermute(value, AXES, [(at(*d), at(*target(*d))) for d in PLACES])


def along(value, axis, step):
    return lax.ppermute(value, axis, [(i, (i + step) % RING) for i in range(RING)])


def other_core(value):
    return lax.ppermute(value, "c", [(0, 1), (1, 0)])


def out_of(shape, dtype):
    return jax.ShapeDtypeStruct(shape, dtype)


def room(mib):
    return pltpu.CompilerParams(vmem_limit_bytes=mib << 20)


def dosage_kernel(dosage_ref, out_ref, totals_ref, acc_ref):
    @pl.when(pl.program_id(0) == 0)
    def _():
        acc_ref[...] = jnp.zeros_like(acc_ref)

    d = dosage_ref[...]
    out_ref[...] = d.astype(jnp.bfloat16)
    groups = d.reshape(d.shape[0] // 8, 8, d.shape[1])
    acc_ref[0:8] += jnp.sum(groups, axis=0)
    acc_ref[8:16] += jnp.sum(groups * groups, axis=0)

    @pl.when(pl.program_id(0) == pl.num_programs(0) - 1)
    def _():
        totals_ref[...] = acc_ref[...].astype(jnp.float32)


def convert_dosage(dosage):
    samples, width = dosage.shape
    block = 512
    return pl.pallas_call(
        dosage_kernel,
        grid=(samples // block,),
        out_shape=(out_of(dosage.shape, jnp.bfloat16), out_of((16, width), jnp.float32)),
        in_specs=[pl.BlockSpec((block, width), lambda i: (i, 0))],
        out_specs=(
            pl.BlockSpec((block, width), lambda i: (i, 0)),
            pl.BlockSpec((16, width), lambda i: (0, 0)),
        ),
        scratch_shapes=[pltpu.VMEM((16, width), jnp.int32)],
        compiler_params=room(8),
    )(dosage)


def table_kernel(*refs):
    blocks, (table_ref, scale_ref, var_ref, code_ref) = refs[:8], refs[8:]
    z, c = lax.axis_index("z"), lax.axis_index("c")
    depth = blocks[0].shape[0]
    count = len(blocks) * blocks[0].size
    values = [r[...] for r in blocks]
    mean = jnp.sum(sum(values)) / count
    values = [v - mean for v in values]
    var_ref[0, 0] = jnp.sum(sum(v * v for v in values)) / count
    rounded = [v.astype(jnp.bfloat16).astype(jnp.float32) for v in values]
    most = jnp.abs(rounded[0])
    for r in rounded[1:]:
        most = jnp.maximum(most, jnp.abs(r))
    most = jnp.full((1, LOW), jnp.maximum(jnp.max(most), 1e-30), jnp.float32)
    for k, r in enumerate(rounded):
        code = jnp.round(jnp.sqrt(jnp.sqrt(jnp.abs(r) / most)) * 32767.0).astype(jnp.int32)
        code = jnp.where(r < 0, -code, code)
        core = c if k < RING else 1 - c
        start = (((z + RING - k % RING) % RING) * 2 + core) * depth
        code_ref[pl.ds(pl.multiple_of(start, 8), depth), :] = code
    half = table_ref.shape[0]
    table_ref[...] = lax.shift_left(code_ref[half:, :], 16) + (code_ref[:half, :] & 0xFFFF)
    scale_ref[...] = jnp.sqrt(jnp.sqrt(most)) / 32767.0


def make_table(blocks):
    rows = len(blocks) * blocks[0].shape[0]
    return pl.pallas_call(
        table_kernel,
        out_shape=(
            out_of((rows // 2, LOW), jnp.int32),
            out_of((1, LOW), jnp.float32),
            out_of((1, 1), jnp.float32),
        ),
        in_specs=[VMEM] * 8,
        out_specs=(VMEM, VMEM, SMEM),
        scratch_shapes=[pltpu.VMEM((rows, LOW), jnp.int32)],
        compiler_params=room(2),
    )(*blocks)


def lookup_kernel(index_ref, table_ref, scale_ref, *rest):
    out_ref = rest[-1]
    rows, width = index_ref.shape
    first = out_ref.shape[0] - rows
    if first:
        out_ref[:first, :] = rest[0][...]
    half = table_ref.shape[0]
    parts = AT_ONCE // (rows // 8)
    span = parts * LOW
    scale = jnp.broadcast_to(scale_ref[...], (8, LOW))

    def step(j, _):
        for part in range(parts):
            base = pl.multiple_of(j * span + part * LOW, LOW)
            found = []
            for i in range(0, rows, 8):
                index = index_ref[pl.ds(i, 8), pl.ds(base, LOW)]
                lane = index & (LOW - 1)
                row = lax.shift_right_logical(index, 7)
                upper = row >= half
                row = jnp.where(upper, row - half, row)
                word = jnp.zeros((8, LOW), jnp.int32)
                for r in range(half):
                    source = jnp.broadcast_to(table_ref[r : r + 1, :], (8, LOW))
                    taken = jnp.take_along_axis(source, lane, axis=1, mode="promise_in_bounds")
                    word = jnp.where(row == r, taken, word)
                code = lax.shift_right_arithmetic(
                    jnp.where(upper, word, lax.shift_left(word, 16)), 16
                )
                root = code.astype(jnp.float32) * scale
                root = root * root
                root = root * root
                found.append(jnp.where(code < 0, -root, root))
            out_ref[first:, pl.ds(base, LOW)] = jnp.concatenate(found, axis=0).astype(jnp.bfloat16)
        return 0

    lax.fori_loop(0, width // span, step, 0)


def lookup(index, k, rows, table, scale, before=()):
    width = index.shape[1]
    shape = (rows + sum(b.shape[0] for b in before), width)
    whole = lambda i: (0, 0)
    return pl.pallas_call(
        lookup_kernel,
        grid=(1,),
        out_shape=out_of(shape, jnp.bfloat16),
        in_specs=[
            pl.BlockSpec((rows, width), lambda i: (k, 0)),
            pl.BlockSpec(table.shape, whole),
            pl.BlockSpec(scale.shape, whole),
        ]
        + [pl.BlockSpec(b.shape, whole) for b in before],
        out_specs=pl.BlockSpec(shape, whole),
        compiler_params=room(3),
    )(index, table, scale, *before)


def ring_gather(value, first, turn):
    def line(sign):
        def target(x, y, z, c):
            step = sign if c == turn else -sign
            if (c == 0) == first:
                return (x + step, y, z, c)
            return (x, y + step, z, c)

        return target

    behind = shift(value, line(1))
    ahead = shift(value, line(-1))
    onward = shift(behind, line(1))
    return [value, behind, ahead, onward]


def offset(k, turn, c):
    step = jnp.where(c == turn, 1, -1)
    return (0, -step, step, 2)[k]


def stack_kernel(a0, a1, a2, a3, out_ref):
    for k, a in enumerate((a0, a1, a2, a3)):
        out_ref[k] = a[...]


def stacked(pieces):
    return pl.pallas_call(
        stack_kernel,
        out_shape=out_of((len(pieces), *pieces[0].shape), pieces[0].dtype),
        in_specs=[VMEM] * 4,
        out_specs=VMEM,
        compiler_params=room(3),
    )(*pieces)


def product_kernel(
    a0, a1, a2, a3, dosage_ref, totals_ref, keep_ref, send_ref, lhs_ref, *, turn_near, turn_far
):
    rows = a0.shape[1]
    extra = keep_ref.shape[1] - 2 * rows
    dest = destinations(turn_near, turn_far)
    for u, a in enumerate((a0, a1, a2, a3)):
        for t in range(RING):
            start = pl.multiple_of(dest(u, t) * rows, rows)
            lhs_ref[pl.ds(start, rows), :] = a[t]
    part = jnp.dot(lhs_ref[...], dosage_ref[...], preferred_element_type=jnp.float32)
    for h, ref in enumerate((keep_ref, send_ref)):
        for k in range(RING):
            start = (h * RING + k) * 2 * rows
            ref[k, : 2 * rows, :] = part[start : start + 2 * rows]
            if extra:
                ref[k, 2 * rows :, :] = totals_ref[...]


def product(pieces, dosage, totals, with_totals, turn_near, turn_far):
    rows = pieces[0].shape[1]
    shape = (RING, 2 * rows + (totals.shape[0] if with_totals else 0), dosage.shape[1])
    return pl.pallas_call(
        lambda *refs: product_kernel(*refs, turn_near=turn_near, turn_far=turn_far),
        out_shape=(out_of(shape, jnp.float32), out_of(shape, jnp.float32)),
        in_specs=[VMEM] * 6,
        out_specs=(VMEM, VMEM),
        scratch_shapes=[pltpu.VMEM((rows * RING * RING, dosage.shape[0]), jnp.bfloat16)],
        compiler_params=room(20),
    )(*pieces, dosage, totals)


def add_kernel(a_ref, b_ref, o0, o1, o2, o3):
    for k, o in enumerate((o0, o1, o2, o3)):
        o[...] = a_ref[k] + b_ref[k]


def core_sum(keep, got):
    one = out_of(keep.shape[1:], jnp.float32)
    return pl.pallas_call(
        add_kernel,
        out_shape=(one,) * 4,
        in_specs=[VMEM] * 2,
        out_specs=(VMEM,) * 4,
        compiler_params=room(4),
    )(keep, got)


def destinations(turn_near, turn_far):
    x, y, z, c = (lax.axis_index(a) for a in AXES)
    step = 1 - 2 * c

    def of(u, t):
        far, near = offset(u, turn_far, c), offset(t, turn_near, c)
        px = (x + RING + jnp.where(c == 0, near, far)) % RING
        py = (y + RING + jnp.where(c == 0, far, near)) % RING
        away = jnp.where(py // 2 == c, 0, 1)
        owner = ((1 - 2 * away) * step * (px - z) + 2 * RING) % RING
        return away * 8 + owner * 2 + py % 2

    return of


def z_line(sign):
    def target(x, y, z, c):
        return (x, y, z + (sign if c == 0 else -sign), c)

    return target


def reduced(keep, send):
    got = other_core(send)
    own, ahead, opposite, behind = core_sum(keep, got)
    passing = shift(opposite, z_line(1))
    from_ahead = shift(behind, z_line(-1))
    from_behind = shift(ahead + passing, z_line(1))
    return own, from_behind, from_ahead


def final_kernel(*refs, extra, count):
    if extra:
        var_ref, end_ref, p, q, r, z_ref, most_ref, inverse_ref = refs
        rows = (p.shape[0] - extra) // 2
        totals = p[2 * rows :, :] + q[2 * rows :, :] + r[2 * rows :, :]
        allele_sum = jnp.sum(totals[0:8], axis=0, keepdims=True)
        allele_sq = jnp.sum(totals[8:16], axis=0, keepdims=True)
        allele_var = allele_sq / count - (allele_sum / count) ** 2
        inverse = 1.0 / jnp.sqrt(count * (var_ref[0, 0] + EPSILON) * (allele_var + EPSILON))
        inverse_ref[...] = inverse
        places = [0, rows]
    else:
        end_ref, inverse_ref, z0, most0, p, q, r, z_ref, most_ref = refs
        rows = p.shape[0] // 2
        inverse = inverse_ref[...]
        for h in range(2):
            z_ref[2 * h * rows : (2 * h + 1) * rows, :] = z0[h * rows : (h + 1) * rows, :]
            most_ref[2 * h * rows : (2 * h + 1) * rows, :] = most0[h * rows : (h + 1) * rows, :]
        places = [rows, 3 * rows]
    width = z_ref.shape[1]
    ends = end_ref[...]
    clipped = jnp.clip(ends, 0, width - 1)
    both = 2 * rows
    z = (p[:both, :] + q[:both, :] + r[:both, :]) * inverse
    lanes = lax.broadcasted_iota(jnp.int32, (both, LOW), 1)
    lane = jnp.broadcast_to(clipped % LOW, (both, LOW))
    group = jnp.broadcast_to(clipped // LOW, (both, LOW))
    parts = [jnp.abs(z[:, g * LOW : (g + 1) * LOW]) for g in range(width // LOW)]
    wholes = [jnp.max(v, axis=1, keepdims=True) for v in parts]
    step = 1
    while step < LOW:
        parts = [
            jnp.maximum(v, jnp.where(lanes >= step, pltpu.roll(v, step, 1), 0.0)) for v in parts
        ]
        step *= 2
    chosen = jnp.zeros((both, LOW), jnp.float32)
    before = jnp.zeros((both, 1), jnp.float32)
    for g, v in enumerate(parts):
        taken = jnp.take_along_axis(v, lane, axis=1, mode="promise_in_bounds")
        chosen = jnp.where(group == g, jnp.maximum(taken, before), chosen)
        before = jnp.maximum(before, wholes[g])
    chosen = jnp.where(jnp.broadcast_to(ends >= 0, (both, LOW)), chosen, 0.0)
    for h, place in enumerate(places):
        z_ref[place : place + rows, :] = z[h * rows : (h + 1) * rows]
        most_ref[place : place + rows, :] = chosen[h * rows : (h + 1) * rows]


def final_first(pheno_var, ends, parts, extra, count):
    rows, width = parts[0].shape[0] - extra, parts[0].shape[1]
    return pl.pallas_call(
        lambda *refs: final_kernel(*refs, extra=extra, count=count),
        out_shape=(
            out_of((rows, width), jnp.float32),
            out_of((rows, ends.shape[1]), jnp.float32),
            out_of((1, width), jnp.float32),
        ),
        in_specs=[SMEM] + [VMEM] * 4,
        out_specs=(VMEM,) * 3,
        compiler_params=room(4),
    )(pheno_var, ends, *parts)


def final_second(ends, inverse, z0, most0, parts, count):
    rows, width = parts[0].shape
    return pl.pallas_call(
        lambda *refs: final_kernel(*refs, extra=0, count=count),
        out_shape=(
            out_of((CHUNKS * rows, width), jnp.float32),
            out_of((CHUNKS * rows, ends.shape[1]), jnp.float32),
        ),
        in_specs=[VMEM] * 7,
        out_specs=(VMEM,) * 2,
        compiler_params=room(4),
    )(ends, inverse, z0, most0, *parts)


def largest(value, first):
    def line(step):
        def target(x, y, z, c):
            return (x + step, y, z, c) if (c == 0) == first else (x, y + step, z, c)

        return target

    got = [shift(value, line(k)) for k in (2, 1, 3)]
    return jnp.maximum(jnp.maximum(value, got[0]), jnp.maximum(got[1], got[2]))


def per_device(dosage, phenotype, perm_index, seg_lengths):
    samples, width = dosage.shape
    x, y = lax.axis_index("x"), lax.axis_index("y")
    own = phenotype.reshape(-1, LOW)
    mine = [own] + [along(own, "z", k) for k in (1, 2, 3)]
    dosage_bf, totals = convert_dosage(dosage)
    table, scale, pheno_var = make_table(mine + [other_core(m) for m in mine])
    ends = (jnp.cumsum(seg_lengths) - 1 - (x * RING + y) * width)[None, :].astype(jnp.int32)
    count = float(samples * lax.axis_size("z") * lax.axis_size("c"))

    rows = perm_index.shape[0] // CHUNKS
    part = rows // 2
    traits = lookup(perm_index, 0, rows, table, scale)
    near = ring_gather(traits, True, 0)
    traits = lookup(perm_index, 2, part, table, scale)
    traits = lookup(perm_index, 3, part, table, scale, (traits,))
    far = ring_gather(stacked(near), False, 1)
    near = ring_gather(traits, True, 1)
    keep, send = product(far, dosage_bf, totals, True, 0, 1)
    parts = reduced(keep, send)
    z0, most0, inverse = final_first(pheno_var, ends, parts, totals.shape[0], count)

    far = ring_gather(stacked(near), False, 0)
    keep, send = product(far, dosage_bf, totals, False, 1, 0)
    parts = reduced(keep, send)
    zscore, most = final_second(ends, inverse, z0, most0, parts, count)
    return (zscore, largest(largest(most, True), False))


def solution(mesh):
    fine = Mesh(mesh.devices.reshape(RING, RING, RING, 2), AXES)
    var, samp = ("x", "y"), ("z", "c")
    return jax.shard_map(
        per_device,
        mesh=fine,
        in_specs=(P(samp, var), P(samp), P(var, samp), P()),
        out_specs=(P(samp, var), P(samp, None)),
        check_vma=False,
    )
```

```python
import jax
import jax.numpy as jnp
from jax import lax
from jax.experimental import pallas as pl
from jax.experimental.pallas import tpu as pltpu
from jax.sharding import Mesh, PartitionSpec as P


EPSILON = 1e-05
RING = 4
AXES = ("x", "y", "z", "c")
CHUNKS = 2
LOW = 128
AT_ONCE = 24
PLACES = [
    (x, y, z, c) for x in range(RING) for y in range(RING) for z in range(RING) for c in range(2)
]
VMEM = pl.BlockSpec(memory_space=pltpu.VMEM)
SMEM = pl.BlockSpec(memory_space=pltpu.SMEM)


def at(x, y, z, c):
    return (((x % RING) * RING + y % RING) * RING + z % RING) * 2 + c


def shift(value, target):
    return lax.ppermute(value, AXES, [(at(*d), at(*target(*d))) for d in PLACES])


def along(value, axis, step):
    return lax.ppermute(value, axis, [(i, (i + step) % RING) for i in range(RING)])


def other_core(value):
    return lax.ppermute(value, "c", [(0, 1), (1, 0)])


def out_of(shape, dtype):
    return jax.ShapeDtypeStruct(shape, dtype)


def room(mib):
    return pltpu.CompilerParams(vmem_limit_bytes=mib << 20)


def dosage_kernel(dosage_ref, out_ref, totals_ref, acc_ref):
    @pl.when(pl.program_id(0) == 0)
    def _():
        acc_ref[...] = jnp.zeros_like(acc_ref)

    d = dosage_ref[...]
    out_ref[...] = d.astype(jnp.bfloat16)
    groups = d.reshape(d.shape[0] // 8, 8, d.shape[1])
    acc_ref[0:8] += jnp.sum(groups, axis=0)
    acc_ref[8:16] += jnp.sum(groups * groups, axis=0)

    @pl.when(pl.program_id(0) == pl.num_programs(0) - 1)
    def _():
        totals_ref[...] = acc_ref[...].astype(jnp.float32)


def convert_dosage(dosage):
    samples, width = dosage.shape
    block = 512
    return pl.pallas_call(
        dosage_kernel,
        grid=(samples // block,),
        out_shape=(out_of(dosage.shape, jnp.bfloat16), out_of((16, width), jnp.float32)),
        in_specs=[pl.BlockSpec((block, width), lambda i: (i, 0))],
        out_specs=(
            pl.BlockSpec((block, width), lambda i: (i, 0)),
            pl.BlockSpec((16, width), lambda i: (0, 0)),
        ),
        scratch_shapes=[pltpu.VMEM((16, width), jnp.int32)],
        compiler_params=room(8),
    )(dosage)


def table_kernel(pair_ref, mine_ref, theirs_ref, far_ref, other_ref, *rest):
    table_ref, scale_ref, var_ref, code_ref = rest
    z, c = lax.axis_index("z"), lax.axis_index("c")
    step = 1 - 2 * c
    depth = far_ref.shape[0]
    blocks = (
        (pair_ref[:depth], z, c),
        (pair_ref[depth:], z, 1 - c),
        (mine_ref[:depth], z - step, c),
        (mine_ref[depth:], z - step, 1 - c),
        (theirs_ref[:depth], z + step, 1 - c),
        (theirs_ref[depth:], z + step, c),
        (far_ref[...], z + 2, c),
        (other_ref[...], z + 2, 1 - c),
    )
    values = [b[0] for b in blocks]
    count = len(values) * values[0].size
    mean = jnp.sum(sum(values)) / count
    values = [v - mean for v in values]
    var_ref[0, 0] = jnp.sum(sum(v * v for v in values)) / count
    rounded = [v.astype(jnp.bfloat16).astype(jnp.float32) for v in values]
    most = jnp.abs(rounded[0])
    for r in rounded[1:]:
        most = jnp.maximum(most, jnp.abs(r))
    most = jnp.full((1, LOW), jnp.maximum(jnp.max(most), 1e-30), jnp.float32)
    for r, (_, at_z, core) in zip(rounded, blocks):
        code = jnp.round(jnp.sqrt(jnp.sqrt(jnp.abs(r) / most)) * 32767.0).astype(jnp.int32)
        code = jnp.where(r < 0, -code, code)
        start = (((at_z + RING) % RING) * 2 + core) * depth
        code_ref[pl.ds(pl.multiple_of(start, 8), depth), :] = code
    half = table_ref.shape[0]
    table_ref[...] = lax.shift_left(code_ref[half:, :], 16) + (code_ref[:half, :] & 0xFFFF)
    scale_ref[...] = jnp.sqrt(jnp.sqrt(most)) / 32767.0


def make_table(own):
    def line(x, y, z, c):
        return (x, y, z + 1 - 2 * c, c)

    other = other_core(own)
    far = along(own, "z", 2)
    pair = join(own, other)
    mine = shift(pair, line)
    far_other = other_core(far)
    theirs = other_core(mine)
    rows = 2 * RING * own.shape[0]
    return pl.pallas_call(
        table_kernel,
        out_shape=(
            out_of((rows // 2, LOW), jnp.int32),
            out_of((1, LOW), jnp.float32),
            out_of((1, 1), jnp.float32),
        ),
        in_specs=[VMEM] * 5,
        out_specs=(VMEM, VMEM, SMEM),
        scratch_shapes=[pltpu.VMEM((rows, LOW), jnp.int32)],
        compiler_params=room(2),
    )(pair, mine, theirs, far, far_other)


def join_kernel(a_ref, b_ref, out_ref):
    out_ref[: a_ref.shape[0]] = a_ref[...]
    out_ref[a_ref.shape[0] :] = b_ref[...]


def join(a, b):
    return pl.pallas_call(
        join_kernel,
        out_shape=out_of((a.shape[0] + b.shape[0], a.shape[1]), a.dtype),
        in_specs=[VMEM] * 2,
        out_specs=VMEM,
        compiler_params=room(2),
    )(a, b)


def copy_kernel(a_ref, out_ref):
    out_ref[...] = a_ref[...]


def fetched(a):
    return pl.pallas_call(
        copy_kernel,
        out_shape=out_of(a.shape, a.dtype),
        in_specs=[VMEM],
        out_specs=VMEM,
        compiler_params=room(4),
    )(a)


def lookup_kernel(index_ref, table_ref, scale_ref, *rest):
    out_ref = rest[-1]
    rows, width = index_ref.shape
    first = out_ref.shape[0] - rows
    if first:
        out_ref[:first, :] = rest[0][...]
    half = table_ref.shape[0]
    parts = AT_ONCE // (rows // 8)
    span = parts * LOW
    scale = jnp.broadcast_to(scale_ref[...], (8, LOW))

    def step(j, _):
        for part in range(parts):
            base = pl.multiple_of(j * span + part * LOW, LOW)
            found = []
            for i in range(0, rows, 8):
                index = index_ref[pl.ds(i, 8), pl.ds(base, LOW)]
                lane = index & (LOW - 1)
                row = lax.shift_right_logical(index, 7)
                upper = row >= half
                row = jnp.where(upper, row - half, row)
                word = jnp.zeros((8, LOW), jnp.int32)
                for r in range(half):
                    source = jnp.broadcast_to(table_ref[r : r + 1, :], (8, LOW))
                    taken = jnp.take_along_axis(source, lane, axis=1, mode="promise_in_bounds")
                    word = jnp.where(row == r, taken, word)
                code = lax.shift_right_arithmetic(
                    jnp.where(upper, word, lax.shift_left(word, 16)), 16
                )
                root = code.astype(jnp.float32) * scale
                root = root * root
                root = root * root
                found.append(jnp.where(code < 0, -root, root))
            out_ref[first:, pl.ds(base, LOW)] = jnp.concatenate(found, axis=0).astype(jnp.bfloat16)
        return 0

    lax.fori_loop(0, width // span, step, 0)


def lookup(index, k, rows, table, scale, before=()):
    width = index.shape[1]
    shape = (rows + sum(b.shape[0] for b in before), width)
    whole = lambda i: (0, 0)
    return pl.pallas_call(
        lookup_kernel,
        grid=(1,),
        out_shape=out_of(shape, jnp.bfloat16),
        in_specs=[
            pl.BlockSpec((rows, width), lambda i: (k, 0)),
            pl.BlockSpec(table.shape, whole),
            pl.BlockSpec(scale.shape, whole),
        ]
        + [pl.BlockSpec(b.shape, whole) for b in before],
        out_specs=pl.BlockSpec(shape, whole),
        compiler_params=room(3),
    )(index, table, scale, *before)


def ring_gather(value, first, turn, dim):
    def line(sign):
        def target(x, y, z, c):
            step = sign if c == turn else -sign
            if (c == 0) == first:
                return (x + step, y, z, c)
            return (x, y + step, z, c)

        return target

    behind = shift(value, line(1))
    ahead = shift(value, line(-1))
    low = shift(half_of(behind, 0, dim), line(1))
    high = shift(half_of(ahead, 1, dim), line(-1))
    return [value, behind, ahead, low, high]


def half_kernel(a_ref, out_ref, *, which, dim):
    size = out_ref.shape[dim]
    part = pl.ds(which * size, size)
    out_ref[...] = a_ref[part] if dim == 0 else a_ref[:, part]


def half_of(a, which, dim):
    shape = tuple(n // 2 if d == dim else n for d, n in enumerate(a.shape))
    return pl.pallas_call(
        lambda *refs: half_kernel(*refs, which=which, dim=dim),
        out_shape=out_of(shape, a.dtype),
        in_specs=[VMEM],
        out_specs=VMEM,
        compiler_params=room(3),
    )(a)


def offset(k, turn, c):
    step = jnp.where(c == turn, 1, -1)
    return (0, -step, step, 2)[k]


def stack_kernel(own, behind, ahead, opposite, out_ref, *, which):
    rows = out_ref.shape[1]
    part = slice(which * rows, (which + 1) * rows)
    for k, a in enumerate((own, behind, ahead)):
        out_ref[k] = a[part, :]
    out_ref[3] = opposite[...]


def stacked(near, which):
    own, behind, ahead = near[:3]
    opposite = near[3 + which]
    return pl.pallas_call(
        lambda *refs: stack_kernel(*refs, which=which),
        out_shape=out_of((RING, *opposite.shape), own.dtype),
        in_specs=[VMEM] * 4,
        out_specs=VMEM,
        compiler_params=room(4),
    )(own, behind, ahead, opposite)


def early_kernel(a0, a1, a2, dosage_ref, out_ref, lhs_ref):
    rows = a0.shape[0] * a0.shape[1]
    for u, a in enumerate((a0, a1, a2)):
        lhs_ref[u * rows : (u + 1) * rows, :] = a[...].reshape(rows, a.shape[2])
    out_ref[...] = jnp.dot(lhs_ref[...], dosage_ref[...], preferred_element_type=jnp.float32)


def early_product(pieces, dosage):
    rows = sum(p.shape[0] * p.shape[1] for p in pieces)
    return pl.pallas_call(
        early_kernel,
        out_shape=out_of((rows, dosage.shape[1]), jnp.float32),
        in_specs=[VMEM] * 4,
        out_specs=VMEM,
        scratch_shapes=[pltpu.VMEM((rows, dosage.shape[0]), jnp.bfloat16)],
        compiler_params=room(16),
    )(*pieces, dosage)


def late_kernel(
    early_ref, low_ref, high_ref, dosage_ref, totals_ref, keep_ref, send_ref, lhs_ref, all_ref,
    *, turn_near, turn_far,
):
    rows = low_ref.shape[1]
    half = low_ref.shape[0] * rows
    extra = keep_ref.shape[1] - 2 * rows
    dest = destinations(turn_near, turn_far)

    def place(u, t, value):
        start = pl.multiple_of(dest(u, t) * rows, rows)
        all_ref[pl.ds(start, rows), :] = value

    lhs_ref[:half, :] = low_ref[...].reshape(half, lhs_ref.shape[1])
    lhs_ref[half:, :] = high_ref[...].reshape(half, lhs_ref.shape[1])
    part = jnp.dot(lhs_ref[...], dosage_ref[...], preferred_element_type=jnp.float32)
    for u in range(RING - 1):
        for t in range(RING):
            start = (u * RING + t) * rows
            place(u, t, early_ref[start : start + rows, :])
    for t in range(RING):
        place(RING - 1, t, part[t * rows : (t + 1) * rows])
    for h, ref in enumerate((keep_ref, send_ref)):
        for k in range(RING):
            start = (h * RING + k) * 2 * rows
            ref[k, : 2 * rows, :] = all_ref[start : start + 2 * rows, :]
            if extra:
                ref[k, 2 * rows :, :] = totals_ref[...]


def late_product(early, low, high, dosage, totals, with_totals, turn_near, turn_far):
    rows = low.shape[1]
    shape = (RING, 2 * rows + (totals.shape[0] if with_totals else 0), dosage.shape[1])
    return pl.pallas_call(
        lambda *refs: late_kernel(*refs, turn_near=turn_near, turn_far=turn_far),
        out_shape=(out_of(shape, jnp.float32), out_of(shape, jnp.float32)),
        in_specs=[VMEM] * 5,
        out_specs=(VMEM, VMEM),
        scratch_shapes=[
            pltpu.VMEM((RING * rows, dosage.shape[0]), jnp.bfloat16),
            pltpu.VMEM((RING * RING * rows, dosage.shape[1]), jnp.float32),
        ],
        compiler_params=room(16),
    )(early, low, high, dosage, totals)


def add_kernel(a_ref, b_ref, o0, o1, o2, o3):
    for k, o in enumerate((o0, o1, o2, o3)):
        o[...] = a_ref[k] + b_ref[k]


def core_sum(keep, got):
    one = out_of(keep.shape[1:], jnp.float32)
    return pl.pallas_call(
        add_kernel,
        out_shape=(one,) * 4,
        in_specs=[VMEM] * 2,
        out_specs=(VMEM,) * 4,
        compiler_params=room(4),
    )(keep, got)


def destinations(turn_near, turn_far):
    x, y, z, c = (lax.axis_index(a) for a in AXES)
    step = 1 - 2 * c

    def of(u, t):
        far, near = offset(u, turn_far, c), offset(t, turn_near, c)
        px = (x + RING + jnp.where(c == 0, near, far)) % RING
        py = (y + RING + jnp.where(c == 0, far, near)) % RING
        away = jnp.where(py // 2 == c, 0, 1)
        owner = ((1 - 2 * away) * step * (px - z) + 2 * RING) % RING
        return away * 8 + owner * 2 + py % 2

    return of


def z_line(sign):
    def target(x, y, z, c):
        return (x, y, z + (sign if c == 0 else -sign), c)

    return target


def reduced(far, dosage, totals, with_totals):
    early = early_product(far[:3], dosage)
    low, high = far[3:]
    keep, send = late_product(early, low, high, dosage, totals, with_totals, 0, 1)
    got = other_core(send)
    own, ahead, opposite, behind = core_sum(keep, got)
    passing = shift(opposite, z_line(1))
    from_ahead = shift(behind, z_line(-1))
    from_behind = shift(ahead + passing, z_line(1))
    return own, from_behind, from_ahead


def final_kernel(*refs, extra, count):
    if extra:
        var_ref, end_ref, p, q, r, z_ref, most_ref, inverse_ref = refs
        rows = (p.shape[0] - extra) // 2
        totals = p[2 * rows :, :] + q[2 * rows :, :] + r[2 * rows :, :]
        allele_sum = jnp.sum(totals[0:8], axis=0, keepdims=True)
        allele_sq = jnp.sum(totals[8:16], axis=0, keepdims=True)
        allele_var = allele_sq / count - (allele_sum / count) ** 2
        inverse = 1.0 / jnp.sqrt(count * (var_ref[0, 0] + EPSILON) * (allele_var + EPSILON))
        inverse_ref[...] = inverse
        places = [0, rows]
    else:
        end_ref, inverse_ref, z0, most0, p, q, r, z_ref, most_ref = refs
        rows = p.shape[0] // 2
        inverse = inverse_ref[...]
        for h in range(2):
            z_ref[2 * h * rows : (2 * h + 1) * rows, :] = z0[h * rows : (h + 1) * rows, :]
            most_ref[2 * h * rows : (2 * h + 1) * rows, :] = most0[h * rows : (h + 1) * rows, :]
        places = [rows, 3 * rows]
    width = z_ref.shape[1]
    ends = end_ref[...]
    clipped = jnp.clip(ends, 0, width - 1)
    both = 2 * rows
    z = (p[:both, :] + q[:both, :] + r[:both, :]) * inverse
    lanes = lax.broadcasted_iota(jnp.int32, (both, LOW), 1)
    lane = jnp.broadcast_to(clipped % LOW, (both, LOW))
    group = jnp.broadcast_to(clipped // LOW, (both, LOW))
    parts = [jnp.abs(z[:, g * LOW : (g + 1) * LOW]) for g in range(width // LOW)]
    wholes = [jnp.max(v, axis=1, keepdims=True) for v in parts]
    step = 1
    while step < LOW:
        parts = [
            jnp.maximum(v, jnp.where(lanes >= step, pltpu.roll(v, step, 1), 0.0)) for v in parts
        ]
        step *= 2
    chosen = jnp.zeros((both, LOW), jnp.float32)
    before = jnp.zeros((both, 1), jnp.float32)
    for g, v in enumerate(parts):
        taken = jnp.take_along_axis(v, lane, axis=1, mode="promise_in_bounds")
        chosen = jnp.where(group == g, jnp.maximum(taken, before), chosen)
        before = jnp.maximum(before, wholes[g])
    chosen = jnp.where(jnp.broadcast_to(ends >= 0, (both, LOW)), chosen, 0.0)
    for h, place in enumerate(places):
        z_ref[place : place + rows, :] = z[h * rows : (h + 1) * rows]
        most_ref[place : place + rows, :] = chosen[h * rows : (h + 1) * rows].astype(most_ref.dtype)


def final_first(pheno_var, ends, parts, extra, count):
    rows, width = parts[0].shape[0] - extra, parts[0].shape[1]
    return pl.pallas_call(
        lambda *refs: final_kernel(*refs, extra=extra, count=count),
        out_shape=(
            out_of((rows, width), jnp.float32),
            out_of((rows, ends.shape[1]), jnp.bfloat16),
            out_of((1, width), jnp.float32),
        ),
        in_specs=[SMEM] + [VMEM] * 4,
        out_specs=(VMEM,) * 3,
        compiler_params=room(4),
    )(pheno_var, ends, *parts)


def final_second(ends, inverse, z0, most0, parts, count):
    rows, width = parts[0].shape
    return pl.pallas_call(
        lambda *refs: final_kernel(*refs, extra=0, count=count),
        out_shape=(
            out_of((CHUNKS * rows, width), jnp.float32),
            out_of((CHUNKS * rows, ends.shape[1]), jnp.bfloat16),
        ),
        in_specs=[VMEM] * 7,
        out_specs=(VMEM,) * 2,
        compiler_params=room(4),
    )(ends, inverse, z0, most0, *parts)


def largest(value, first):
    def line(step):
        def target(x, y, z, c):
            return (x + step, y, z, c) if (c == 0) == first else (x, y + step, z, c)

        return target

    got = [shift(value, line(k)) for k in (2, 1, 3)]
    return jnp.maximum(jnp.maximum(value, got[0]), jnp.maximum(got[1], got[2]))


def per_device(dosage, phenotype, perm_index, seg_lengths):
    samples, width = dosage.shape
    x, y = lax.axis_index("x"), lax.axis_index("y")
    perm_index = fetched(perm_index)
    dosage_bf, totals = convert_dosage(dosage)
    table, scale, pheno_var = make_table(phenotype.reshape(-1, LOW))
    ends = (jnp.cumsum(seg_lengths) - 1 - (x * RING + y) * width)[None, :].astype(jnp.int32)
    count = float(samples * lax.axis_size("z") * lax.axis_size("c"))

    traits = lookup(perm_index, 0, perm_index.shape[0], table, scale)
    near = ring_gather(traits, True, 0, 0)
    far = [ring_gather(stacked(near, k), False, 1, 0) for k in range(CHUNKS)]
    parts = reduced(far[0], dosage_bf, totals, True)
    z0, most0, inverse = final_first(pheno_var, ends, parts, totals.shape[0], count)
    parts = reduced(far[1], dosage_bf, totals, False)
    zscore, most = final_second(ends, inverse, z0, most0, parts, count)
    return (zscore, largest(largest(most, True), False).astype(jnp.float32))


def solution(mesh):
    fine = Mesh(mesh.devices.reshape(RING, RING, RING, 2), AXES)
    var, samp = ("x", "y"), ("z", "c")
    return jax.shard_map(
        per_device,
        mesh=fine,
        in_specs=(P(samp, var), P(samp), P(var, samp), P()),
        out_specs=(P(samp, var), P(samp, None)),
        check_vma=False,
    )
```

```python
import jax
import jax.numpy as jnp
from jax import lax
from jax.experimental import pallas as pl
from jax.experimental.pallas import tpu as pltpu
from jax.sharding import Mesh, PartitionSpec as P


EPSILON = 1e-05
RING = 4
AXES = ("x", "y", "z", "c")
CHUNKS = 2
LOW = 128
COLUMNS = 3
PLACES = [
    (x, y, z, c) for x in range(RING) for y in range(RING) for z in range(RING) for c in range(2)
]
VMEM = pl.BlockSpec(memory_space=pltpu.VMEM)
SMEM = pl.BlockSpec(memory_space=pltpu.SMEM)


def at(x, y, z, c):
    return (((x % RING) * RING + y % RING) * RING + z % RING) * 2 + c


def shift(value, target):
    return lax.ppermute(value, AXES, [(at(*d), at(*target(*d))) for d in PLACES])


def along(value, axis, step):
    return lax.ppermute(value, axis, [(i, (i + step) % RING) for i in range(RING)])


def other_core(value):
    return lax.ppermute(value, "c", [(0, 1), (1, 0)])


def out_of(shape, dtype):
    return jax.ShapeDtypeStruct(shape, dtype)


def room(mib):
    return pltpu.CompilerParams(vmem_limit_bytes=mib << 20)


def dosage_kernel(dosage_ref, out_ref, totals_ref, acc_ref):
    @pl.when(pl.program_id(0) == 0)
    def _():
        acc_ref[...] = jnp.zeros_like(acc_ref)

    d = dosage_ref[...]
    out_ref[...] = d.astype(jnp.bfloat16)
    groups = d.reshape(d.shape[0] // 8, 8, d.shape[1])
    acc_ref[0:8] += jnp.sum(groups, axis=0)
    acc_ref[8:16] += jnp.sum(groups * groups, axis=0)

    @pl.when(pl.program_id(0) == pl.num_programs(0) - 1)
    def _():
        totals_ref[...] = acc_ref[...].astype(jnp.float32)


def convert_dosage(dosage):
    samples, width = dosage.shape
    block = 512
    return pl.pallas_call(
        dosage_kernel,
        grid=(samples // block,),
        out_shape=(out_of(dosage.shape, jnp.bfloat16), out_of((16, width), jnp.float32)),
        in_specs=[pl.BlockSpec((block, width), lambda i: (i, 0))],
        out_specs=(
            pl.BlockSpec((block, width), lambda i: (i, 0)),
            pl.BlockSpec((16, width), lambda i: (0, 0)),
        ),
        scratch_shapes=[pltpu.VMEM((16, width), jnp.int32)],
        compiler_params=room(8),
    )(dosage)


def table_kernel(pair_ref, mine_ref, theirs_ref, far_ref, other_ref, *rest):
    table_ref, scale_ref, var_ref, plain_ref, code_ref, value_ref = rest
    z, c = lax.axis_index("z"), lax.axis_index("c")
    step = 1 - 2 * c
    depth = far_ref.shape[0]
    blocks = (
        (pair_ref[:depth], z, c),
        (pair_ref[depth:], z, 1 - c),
        (mine_ref[:depth], z - step, c),
        (mine_ref[depth:], z - step, 1 - c),
        (theirs_ref[:depth], z + step, 1 - c),
        (theirs_ref[depth:], z + step, c),
        (far_ref[...], z + 2, c),
        (other_ref[...], z + 2, 1 - c),
    )
    values = [b[0] for b in blocks]
    count = len(values) * values[0].size
    mean = jnp.sum(sum(values)) / count
    values = [v - mean for v in values]
    var_ref[0, 0] = jnp.sum(sum(v * v for v in values)) / count
    rounded = [v.astype(jnp.bfloat16).astype(jnp.float32) for v in values]
    most = jnp.abs(rounded[0])
    for r in rounded[1:]:
        most = jnp.maximum(most, jnp.abs(r))
    most = jnp.full((1, LOW), jnp.maximum(jnp.max(most), 1e-30), jnp.float32)
    for r, (_, at_z, core) in zip(rounded, blocks):
        code = jnp.round(jnp.sqrt(jnp.sqrt(jnp.abs(r) / most)) * 32767.0).astype(jnp.int32)
        code = jnp.where(r < 0, -code, code)
        start = pl.multiple_of((((at_z + RING) % RING) * 2 + core) * depth, 8)
        code_ref[pl.ds(start, depth), :] = code
        value_ref[pl.ds(start, depth), :] = r
    half = table_ref.shape[0]
    plain_ref[:, :LOW] = value_ref[:half, :].astype(jnp.bfloat16)
    plain_ref[:, LOW:] = value_ref[half:, :].astype(jnp.bfloat16)
    table_ref[...] = lax.shift_left(code_ref[half:, :], 16) + (code_ref[:half, :] & 0xFFFF)
    scale_ref[...] = jnp.sqrt(jnp.sqrt(most)) / 32767.0


def make_table(own):
    def line(x, y, z, c):
        return (x, y, z + 1 - 2 * c, c)

    other = other_core(own)
    far = along(own, "z", 2)
    pair = join(own, other)
    mine = shift(pair, line)
    far_other = other_core(far)
    theirs = other_core(mine)
    rows = 2 * RING * own.shape[0]
    return pl.pallas_call(
        table_kernel,
        out_shape=(
            out_of((rows // 2, LOW), jnp.int32),
            out_of((1, LOW), jnp.float32),
            out_of((1, 1), jnp.float32),
            out_of((rows // 2, 2 * LOW), jnp.bfloat16),
        ),
        in_specs=[VMEM] * 5,
        out_specs=(VMEM, VMEM, SMEM, VMEM),
        scratch_shapes=[pltpu.VMEM((rows, LOW), jnp.int32), pltpu.VMEM((rows, LOW), jnp.float32)],
        compiler_params=room(2),
    )(pair, mine, theirs, far, far_other)


def join_kernel(a_ref, b_ref, out_ref):
    out_ref[: a_ref.shape[0]] = a_ref[...]
    out_ref[a_ref.shape[0] :] = b_ref[...]


def join(a, b):
    return pl.pallas_call(
        join_kernel,
        out_shape=out_of((a.shape[0] + b.shape[0], a.shape[1]), a.dtype),
        in_specs=[VMEM] * 2,
        out_specs=VMEM,
        compiler_params=room(2),
    )(a, b)


def copy_kernel(a_ref, out_ref):
    out_ref[...] = a_ref[...]


def fetched(a):
    return pl.pallas_call(
        copy_kernel,
        out_shape=out_of(a.shape, a.dtype),
        in_specs=[VMEM],
        out_specs=VMEM,
        compiler_params=room(4),
    )(a)


def places_of(index, half):
    row = lax.shift_right_logical(index, 7)
    upper = row >= half
    return index & (LOW - 1), jnp.where(upper, row - half, row), upper


def by_gathers(index, table_ref, scale):
    half = table_ref.shape[0]
    lane, row, upper = places_of(index, half)
    word = jnp.zeros((8, LOW), jnp.int32)
    for r in range(half):
        source = jnp.broadcast_to(table_ref[r : r + 1, :], (8, LOW))
        taken = jnp.take_along_axis(source, lane, axis=1, mode="promise_in_bounds")
        word = jnp.where(row == r, taken, word)
        yield None
    code = lax.shift_right_arithmetic(jnp.where(upper, word, lax.shift_left(word, 16)), 16)
    root = code.astype(jnp.float32) * scale
    root = root * root
    root = root * root
    yield jnp.where(code < 0, -root, root)


def by_products(index, plain_ref, lane_ref, row_ref):
    half = plain_ref.shape[0]
    lane, row, upper = places_of(index, half)
    lane_ref[...] = jnp.where(upper, lane + LOW, lane).astype(jnp.float32)
    row_ref[...] = row
    one = jnp.ones((16, LOW), jnp.bfloat16)
    zero = jnp.zeros((16, LOW), jnp.bfloat16)
    along_16 = lax.broadcasted_iota(jnp.int32, (16, LOW), 0).astype(jnp.float32)
    along_16 = along_16.astype(jnp.bfloat16)
    along_8 = lax.broadcasted_iota(jnp.int32, (8, LOW), 0)
    found = []
    for i in range(0, 8, 2):
        columns = []
        for j in (i, i + 1):
            want = jnp.broadcast_to(lane_ref[j : j + 1, :], (16, LOW)).astype(jnp.bfloat16)
            hot = [
                jnp.where(want == along_16 + jnp.bfloat16(16 * k), one, zero)
                for k in range(2 * LOW // 16)
            ]
            columns.append(jnp.concatenate(hot, axis=0))
        picked = jnp.dot(
            plain_ref[...], jnp.concatenate(columns, axis=1), preferred_element_type=jnp.float32
        )
        for part, j in enumerate((i, i + 1)):
            want = jnp.broadcast_to(row_ref[j : j + 1, :], (8, LOW))
            value = jnp.zeros((8, LOW), jnp.float32)
            for q in range(half // 8):
                here = picked[8 * q : 8 * q + 8, part * LOW : (part + 1) * LOW]
                value = jnp.where(want == along_8 + 8 * q, here, value)
            found.append(jnp.sum(value, axis=0, keepdims=True))
        yield None
    yield jnp.concatenate(found, axis=0)


def lookup_kernel(index_ref, table_ref, scale_ref, plain_ref, out_ref, found_ref, lane_ref, row_ref):
    rows, width = index_ref.shape
    groups = rows // 8
    scale = jnp.broadcast_to(scale_ref[...], (8, LOW))
    units = COLUMNS * groups
    dotted = units // 2

    def step(t, _):
        base = pl.multiple_of(t * COLUMNS * LOW, LOW)

        def work(unit):
            column, i = unit // groups, unit % groups * 8
            index = index_ref[i : i + 8, pl.ds(base + column * LOW, LOW)]
            if unit < dotted:
                steps = by_products(index, plain_ref, lane_ref.at[unit], row_ref.at[unit])
            else:
                steps = by_gathers(index, table_ref, scale)
            for value in steps:
                if value is not None:
                    found_ref[i : i + 8, column * LOW : (column + 1) * LOW] = value
                yield

        products = [work(u) for u in range(dotted)]
        gathers = [work(u) for u in range(dotted, units)]
        first = (None for g in products for _ in g)
        second = (None for g in gathers for _ in g)
        fine = table_ref.shape[0] + 1
        for k in range((units - dotted) * fine):
            next(second, None)
            if k % (fine // 5) == 0:
                next(first, None)
        for _ in first:
            pass
        for _ in second:
            pass
        out_ref[:, pl.ds(base, COLUMNS * LOW)] = found_ref[...].astype(jnp.bfloat16)
        return 0

    lax.fori_loop(0, width // (COLUMNS * LOW), step, 0)


def lookup(index, table, scale, plain):
    groups = index.shape[0] // 8
    slots = (COLUMNS * groups // 2, 8, LOW)
    return pl.pallas_call(
        lookup_kernel,
        out_shape=out_of(index.shape, jnp.bfloat16),
        in_specs=[VMEM] * 4,
        out_specs=VMEM,
        scratch_shapes=[
            pltpu.VMEM((index.shape[0], COLUMNS * LOW), jnp.float32),
            pltpu.VMEM(slots, jnp.float32),
            pltpu.VMEM(slots, jnp.int32),
        ],
        compiler_params=room(6),
    )(index, table, scale, plain)


def ring_gather(value, first, turn, dim):
    def line(sign):
        def target(x, y, z, c):
            step = sign if c == turn else -sign
            if (c == 0) == first:
                return (x + step, y, z, c)
            return (x, y + step, z, c)

        return target

    behind = shift(value, line(1))
    ahead = shift(value, line(-1))
    low = shift(half_of(behind, 0, dim), line(1))
    high = shift(half_of(ahead, 1, dim), line(-1))
    return [value, behind, ahead, low, high]


def half_kernel(a_ref, out_ref, *, which, dim):
    size = out_ref.shape[dim]
    part = pl.ds(which * size, size)
    out_ref[...] = a_ref[part] if dim == 0 else a_ref[:, part]


def half_of(a, which, dim):
    shape = tuple(n // 2 if d == dim else n for d, n in enumerate(a.shape))
    return pl.pallas_call(
        lambda *refs: half_kernel(*refs, which=which, dim=dim),
        out_shape=out_of(shape, a.dtype),
        in_specs=[VMEM],
        out_specs=VMEM,
        compiler_params=room(3),
    )(a)


def offset(k, turn, c):
    step = jnp.where(c == turn, 1, -1)
    return (0, -step, step, 2)[k]


def stack_kernel(own, behind, ahead, opposite, out_ref, *, which):
    rows = out_ref.shape[1]
    part = slice(which * rows, (which + 1) * rows)
    for k, a in enumerate((own, behind, ahead)):
        out_ref[k] = a[part, :]
    out_ref[3] = opposite[...]


def stacked(near, which):
    own, behind, ahead = near[:3]
    opposite = near[3 + which]
    return pl.pallas_call(
        lambda *refs: stack_kernel(*refs, which=which),
        out_shape=out_of((RING, *opposite.shape), own.dtype),
        in_specs=[VMEM] * 4,
        out_specs=VMEM,
        compiler_params=room(4),
    )(own, behind, ahead, opposite)


def early_kernel(a0, a1, a2, dosage_ref, out_ref, lhs_ref):
    rows = a0.shape[0] * a0.shape[1]
    for u, a in enumerate((a0, a1, a2)):
        lhs_ref[u * rows : (u + 1) * rows, :] = a[...].reshape(rows, a.shape[2])
    out_ref[...] = jnp.dot(lhs_ref[...], dosage_ref[...], preferred_element_type=jnp.float32)


def early_product(pieces, dosage):
    rows = sum(p.shape[0] * p.shape[1] for p in pieces)
    return pl.pallas_call(
        early_kernel,
        out_shape=out_of((rows, dosage.shape[1]), jnp.float32),
        in_specs=[VMEM] * 4,
        out_specs=VMEM,
        scratch_shapes=[pltpu.VMEM((rows, dosage.shape[0]), jnp.bfloat16)],
        compiler_params=room(16),
    )(*pieces, dosage)


def late_kernel(
    early_ref, low_ref, high_ref, dosage_ref, totals_ref, keep_ref, send_ref, lhs_ref, all_ref,
    *, turn_near, turn_far,
):
    rows = low_ref.shape[1]
    half = low_ref.shape[0] * rows
    extra = keep_ref.shape[1] - 2 * rows
    dest = destinations(turn_near, turn_far)

    def place(u, t, value):
        start = pl.multiple_of(dest(u, t) * rows, rows)
        all_ref[pl.ds(start, rows), :] = value

    lhs_ref[:half, :] = low_ref[...].reshape(half, lhs_ref.shape[1])
    lhs_ref[half:, :] = high_ref[...].reshape(half, lhs_ref.shape[1])
    part = jnp.dot(lhs_ref[...], dosage_ref[...], preferred_element_type=jnp.float32)
    for u in range(RING - 1):
        for t in range(RING):
            start = (u * RING + t) * rows
            place(u, t, early_ref[start : start + rows, :])
    for t in range(RING):
        place(RING - 1, t, part[t * rows : (t + 1) * rows])
    for h, ref in enumerate((keep_ref, send_ref)):
        for k in range(RING):
            start = (h * RING + k) * 2 * rows
            ref[k, : 2 * rows, :] = all_ref[start : start + 2 * rows, :]
            if extra:
                ref[k, 2 * rows :, :] = totals_ref[...]


def late_product(early, low, high, dosage, totals, with_totals, turn_near, turn_far):
    rows = low.shape[1]
    shape = (RING, 2 * rows + (totals.shape[0] if with_totals else 0), dosage.shape[1])
    return pl.pallas_call(
        lambda *refs: late_kernel(*refs, turn_near=turn_near, turn_far=turn_far),
        out_shape=(out_of(shape, jnp.float32), out_of(shape, jnp.float32)),
        in_specs=[VMEM] * 5,
        out_specs=(VMEM, VMEM),
        scratch_shapes=[
            pltpu.VMEM((RING * rows, dosage.shape[0]), jnp.bfloat16),
            pltpu.VMEM((RING * RING * rows, dosage.shape[1]), jnp.float32),
        ],
        compiler_params=room(16),
    )(early, low, high, dosage, totals)


def add_kernel(a_ref, b_ref, o0, o1, o2, o3):
    for k, o in enumerate((o0, o1, o2, o3)):
        o[...] = a_ref[k] + b_ref[k]


def core_sum(keep, got):
    one = out_of(keep.shape[1:], jnp.float32)
    return pl.pallas_call(
        add_kernel,
        out_shape=(one,) * 4,
        in_specs=[VMEM] * 2,
        out_specs=(VMEM,) * 4,
        compiler_params=room(4),
    )(keep, got)


def destinations(turn_near, turn_far):
    x, y, z, c = (lax.axis_index(a) for a in AXES)
    step = 1 - 2 * c

    def of(u, t):
        far, near = offset(u, turn_far, c), offset(t, turn_near, c)
        px = (x + RING + jnp.where(c == 0, near, far)) % RING
        py = (y + RING + jnp.where(c == 0, far, near)) % RING
        away = jnp.where(py // 2 == c, 0, 1)
        owner = ((1 - 2 * away) * step * (px - z) + 2 * RING) % RING
        return away * 8 + owner * 2 + py % 2

    return of


def z_line(sign):
    def target(x, y, z, c):
        return (x, y, z + (sign if c == 0 else -sign), c)

    return target


def reduced(far, dosage, totals, with_totals):
    early = early_product(far[:3], dosage)
    low, high = far[3:]
    keep, send = late_product(early, low, high, dosage, totals, with_totals, 0, 1)
    got = other_core(send)
    own, ahead, opposite, behind = core_sum(keep, got)
    passing = shift(opposite, z_line(1))
    from_ahead = shift(behind, z_line(-1))
    from_behind = shift(ahead + passing, z_line(1))
    return own, from_behind, from_ahead


def final_kernel(*refs, extra, count):
    if extra:
        var_ref, end_ref, p, q, r, z_ref, most_ref, inverse_ref = refs
        rows = (p.shape[0] - extra) // 2
        totals = p[2 * rows :, :] + q[2 * rows :, :] + r[2 * rows :, :]
        allele_sum = jnp.sum(totals[0:8], axis=0, keepdims=True)
        allele_sq = jnp.sum(totals[8:16], axis=0, keepdims=True)
        allele_var = allele_sq / count - (allele_sum / count) ** 2
        inverse = 1.0 / jnp.sqrt(count * (var_ref[0, 0] + EPSILON) * (allele_var + EPSILON))
        inverse_ref[...] = inverse
        places = [0, rows]
    else:
        end_ref, inverse_ref, z0, most0, p, q, r, z_ref, most_ref = refs
        rows = p.shape[0] // 2
        inverse = inverse_ref[...]
        for h in range(2):
            z_ref[2 * h * rows : (2 * h + 1) * rows, :] = z0[h * rows : (h + 1) * rows, :]
            most_ref[2 * h * rows : (2 * h + 1) * rows, :] = most0[h * rows : (h + 1) * rows, :]
        places = [rows, 3 * rows]
    width = z_ref.shape[1]
    ends = end_ref[...]
    clipped = jnp.clip(ends, 0, width - 1)
    both = 2 * rows
    z = (p[:both, :] + q[:both, :] + r[:both, :]) * inverse
    lanes = lax.broadcasted_iota(jnp.int32, (both, LOW), 1)
    lane = jnp.broadcast_to(clipped % LOW, (both, LOW))
    group = jnp.broadcast_to(clipped // LOW, (both, LOW))
    parts = [jnp.abs(z[:, g * LOW : (g + 1) * LOW]) for g in range(width // LOW)]
    wholes = [jnp.max(v, axis=1, keepdims=True) for v in parts]
    step = 1
    while step < LOW:
        parts = [
            jnp.maximum(v, jnp.where(lanes >= step, pltpu.roll(v, step, 1), 0.0)) for v in parts
        ]
        step *= 2
    chosen = jnp.zeros((both, LOW), jnp.float32)
    before = jnp.zeros((both, 1), jnp.float32)
    for g, v in enumerate(parts):
        taken = jnp.take_along_axis(v, lane, axis=1, mode="promise_in_bounds")
        chosen = jnp.where(group == g, jnp.maximum(taken, before), chosen)
        before = jnp.maximum(before, wholes[g])
    chosen = jnp.where(jnp.broadcast_to(ends >= 0, (both, LOW)), chosen, 0.0)
    for h, place in enumerate(places):
        z_ref[place : place + rows, :] = z[h * rows : (h + 1) * rows]
        most_ref[place : place + rows, :] = chosen[h * rows : (h + 1) * rows].astype(most_ref.dtype)


def final_first(pheno_var, ends, parts, extra, count):
    rows, width = parts[0].shape[0] - extra, parts[0].shape[1]
    return pl.pallas_call(
        lambda *refs: final_kernel(*refs, extra=extra, count=count),
        out_shape=(
            out_of((rows, width), jnp.float32),
            out_of((rows, ends.shape[1]), jnp.bfloat16),
            out_of((1, width), jnp.float32),
        ),
        in_specs=[SMEM] + [VMEM] * 4,
        out_specs=(VMEM,) * 3,
        compiler_params=room(4),
    )(pheno_var, ends, *parts)


def final_second(ends, inverse, z0, most0, parts, count):
    rows, width = parts[0].shape
    return pl.pallas_call(
        lambda *refs: final_kernel(*refs, extra=0, count=count),
        out_shape=(
            out_of((CHUNKS * rows, width), jnp.float32),
            out_of((CHUNKS * rows, ends.shape[1]), jnp.bfloat16),
        ),
        in_specs=[VMEM] * 7,
        out_specs=(VMEM,) * 2,
        compiler_params=room(4),
    )(ends, inverse, z0, most0, *parts)


def largest(value, first):
    def line(step):
        def target(x, y, z, c):
            return (x + step, y, z, c) if (c == 0) == first else (x, y + step, z, c)

        return target

    got = [shift(value, line(k)) for k in (2, 1, 3)]
    return jnp.maximum(jnp.maximum(value, got[0]), jnp.maximum(got[1], got[2]))


def per_device(dosage, phenotype, perm_index, seg_lengths):
    samples, width = dosage.shape
    x, y = lax.axis_index("x"), lax.axis_index("y")
    perm_index = fetched(perm_index)
    dosage_bf, totals = convert_dosage(dosage)
    table, scale, pheno_var, plain = make_table(phenotype.reshape(-1, LOW))
    ends = (jnp.cumsum(seg_lengths) - 1 - (x * RING + y) * width)[None, :].astype(jnp.int32)
    count = float(samples * lax.axis_size("z") * lax.axis_size("c"))

    traits = lookup(perm_index, table, scale, plain)
    near = ring_gather(traits, True, 0, 0)
    far = [ring_gather(stacked(near, k), False, 1, 0) for k in range(CHUNKS)]
    parts = reduced(far[0], dosage_bf, totals, True)
    z0, most0, inverse = final_first(pheno_var, ends, parts, totals.shape[0], count)
    parts = reduced(far[1], dosage_bf, totals, False)
    zscore, most = final_second(ends, inverse, z0, most0, parts, count)
    return (zscore, largest(largest(most, True), False).astype(jnp.float32))


def solution(mesh):
    fine = Mesh(mesh.devices.reshape(RING, RING, RING, 2), AXES)
    var, samp = ("x", "y"), ("z", "c")
    return jax.shard_map(
        per_device,
        mesh=fine,
        in_specs=(P(samp, var), P(samp), P(var, samp), P()),
        out_specs=(P(samp, var), P(samp, None)),
        check_vma=False,
    )
```

```python
import jax
import jax.numpy as jnp
from jax import lax
from jax.experimental import pallas as pl
from jax.experimental.pallas import tpu as pltpu
from jax.sharding import Mesh, PartitionSpec as P


EPSILON = 1e-05
RING = 4
AXES = ("x", "y", "z", "c")
CHUNKS = 2
LOW = 128
COLUMNS = 6
PLACES = [
    (x, y, z, c) for x in range(RING) for y in range(RING) for z in range(RING) for c in range(2)
]
VMEM = pl.BlockSpec(memory_space=pltpu.VMEM)
SMEM = pl.BlockSpec(memory_space=pltpu.SMEM)


def at(x, y, z, c):
    return (((x % RING) * RING + y % RING) * RING + z % RING) * 2 + c


def shift(value, target):
    return lax.ppermute(value, AXES, [(at(*d), at(*target(*d))) for d in PLACES])


def along(value, axis, step):
    return lax.ppermute(value, axis, [(i, (i + step) % RING) for i in range(RING)])


def other_core(value):
    return lax.ppermute(value, "c", [(0, 1), (1, 0)])


def out_of(shape, dtype):
    return jax.ShapeDtypeStruct(shape, dtype)


def room(mib):
    return pltpu.CompilerParams(vmem_limit_bytes=mib << 20)


def dosage_kernel(dosage_ref, out_ref, totals_ref, acc_ref):
    @pl.when(pl.program_id(0) == 0)
    def _():
        acc_ref[...] = jnp.zeros_like(acc_ref)

    d = dosage_ref[...]
    out_ref[...] = d.astype(jnp.bfloat16)
    groups = d.reshape(d.shape[0] // 8, 8, d.shape[1])
    acc_ref[0:8] += jnp.sum(groups, axis=0)
    acc_ref[8:16] += jnp.sum(groups * groups, axis=0)

    @pl.when(pl.program_id(0) == pl.num_programs(0) - 1)
    def _():
        totals_ref[...] = acc_ref[...].astype(jnp.float32)


def convert_dosage(dosage):
    samples, width = dosage.shape
    block = 512
    return pl.pallas_call(
        dosage_kernel,
        grid=(samples // block,),
        out_shape=(out_of(dosage.shape, jnp.bfloat16), out_of((16, width), jnp.float32)),
        in_specs=[pl.BlockSpec((block, width), lambda i: (i, 0))],
        out_specs=(
            pl.BlockSpec((block, width), lambda i: (i, 0)),
            pl.BlockSpec((16, width), lambda i: (0, 0)),
        ),
        scratch_shapes=[pltpu.VMEM((16, width), jnp.int32)],
        compiler_params=room(8),
    )(dosage)


def table_kernel(pair_ref, mine_ref, theirs_ref, far_ref, other_ref, *rest):
    table_ref, scale_ref, var_ref, plain_ref, code_ref, value_ref = rest
    z, c = lax.axis_index("z"), lax.axis_index("c")
    step = 1 - 2 * c
    depth = far_ref.shape[0]
    blocks = (
        (pair_ref[:depth], z, c),
        (pair_ref[depth:], z, 1 - c),
        (mine_ref[:depth], z - step, c),
        (mine_ref[depth:], z - step, 1 - c),
        (theirs_ref[:depth], z + step, 1 - c),
        (theirs_ref[depth:], z + step, c),
        (far_ref[...], z + 2, c),
        (other_ref[...], z + 2, 1 - c),
    )
    values = [b[0] for b in blocks]
    count = len(values) * values[0].size
    mean = jnp.sum(sum(values)) / count
    values = [v - mean for v in values]
    var_ref[0, 0] = jnp.sum(sum(v * v for v in values)) / count
    rounded = [v.astype(jnp.bfloat16).astype(jnp.float32) for v in values]
    most = jnp.abs(rounded[0])
    for r in rounded[1:]:
        most = jnp.maximum(most, jnp.abs(r))
    most = jnp.full((1, LOW), jnp.maximum(jnp.max(most), 1e-30), jnp.float32)
    for r, (_, at_z, core) in zip(rounded, blocks):
        code = jnp.round(jnp.sqrt(jnp.sqrt(jnp.abs(r) / most)) * 32767.0).astype(jnp.int32)
        code = jnp.where(r < 0, -code, code)
        start = pl.multiple_of((((at_z + RING) % RING) * 2 + core) * depth, 8)
        code_ref[pl.ds(start, depth), :] = code
        value_ref[pl.ds(start, depth), :] = r
    half = table_ref.shape[0]
    plain_ref[:, :LOW] = value_ref[:half, :].astype(jnp.bfloat16)
    plain_ref[:, LOW:] = value_ref[half:, :].astype(jnp.bfloat16)
    table_ref[...] = lax.shift_left(code_ref[half:, :], 16) + (code_ref[:half, :] & 0xFFFF)
    scale_ref[...] = jnp.sqrt(jnp.sqrt(most)) / 32767.0


def make_table(own):
    def line(x, y, z, c):
        return (x, y, z + 1 - 2 * c, c)

    other = other_core(own)
    far = along(own, "z", 2)
    pair = join(own, other)
    mine = shift(pair, line)
    far_other = other_core(far)
    theirs = other_core(mine)
    rows = 2 * RING * own.shape[0]
    return pl.pallas_call(
        table_kernel,
        out_shape=(
            out_of((rows // 2, LOW), jnp.int32),
            out_of((1, LOW), jnp.float32),
            out_of((1, 1), jnp.float32),
            out_of((rows // 2, 2 * LOW), jnp.bfloat16),
        ),
        in_specs=[VMEM] * 5,
        out_specs=(VMEM, VMEM, SMEM, VMEM),
        scratch_shapes=[pltpu.VMEM((rows, LOW), jnp.int32), pltpu.VMEM((rows, LOW), jnp.float32)],
        compiler_params=room(2),
    )(pair, mine, theirs, far, far_other)


def join_kernel(a_ref, b_ref, out_ref):
    out_ref[: a_ref.shape[0]] = a_ref[...]
    out_ref[a_ref.shape[0] :] = b_ref[...]


def join(a, b):
    return pl.pallas_call(
        join_kernel,
        out_shape=out_of((a.shape[0] + b.shape[0], a.shape[1]), a.dtype),
        in_specs=[VMEM] * 2,
        out_specs=VMEM,
        compiler_params=room(2),
    )(a, b)


def fetch_kernel(a_ref, *outs):
    rows = outs[0].shape[0]
    for k, out in enumerate(outs):
        out[...] = a_ref[k * rows : (k + 1) * rows, :]


def fetched(a):
    one = out_of((a.shape[0] // CHUNKS, a.shape[1]), a.dtype)
    return pl.pallas_call(
        fetch_kernel,
        out_shape=(one,) * CHUNKS,
        in_specs=[VMEM],
        out_specs=(VMEM,) * CHUNKS,
        compiler_params=room(4),
    )(a)


def places_of(index, half):
    row = lax.shift_right_logical(index, 7)
    upper = row >= half
    return index & (LOW - 1), jnp.where(upper, row - half, row), upper


def by_gathers(index, table_ref, scale):
    half = table_ref.shape[0]
    lane, row, upper = places_of(index, half)
    word = jnp.zeros((8, LOW), jnp.int32)
    for r in range(half):
        source = jnp.broadcast_to(table_ref[r : r + 1, :], (8, LOW))
        taken = jnp.take_along_axis(source, lane, axis=1, mode="promise_in_bounds")
        word = jnp.where(row == r, taken, word)
        yield None
    code = lax.shift_right_arithmetic(jnp.where(upper, word, lax.shift_left(word, 16)), 16)
    root = code.astype(jnp.float32) * scale
    root = root * root
    root = root * root
    yield jnp.where(code < 0, -root, root)


def by_products(index, plain_ref, lane_ref, row_ref):
    half = plain_ref.shape[0]
    lane, row, upper = places_of(index, half)
    lane_ref[...] = jnp.where(upper, lane + LOW, lane).astype(jnp.float32)
    row_ref[...] = row
    one = jnp.ones((16, LOW), jnp.bfloat16)
    zero = jnp.zeros((16, LOW), jnp.bfloat16)
    along_16 = lax.broadcasted_iota(jnp.int32, (16, LOW), 0).astype(jnp.float32)
    along_16 = along_16.astype(jnp.bfloat16)
    along_8 = lax.broadcasted_iota(jnp.int32, (8, LOW), 0)
    found = []
    for i in range(0, 8, 2):
        columns = []
        for j in (i, i + 1):
            want = jnp.broadcast_to(lane_ref[j : j + 1, :], (16, LOW)).astype(jnp.bfloat16)
            hot = [
                jnp.where(want == along_16 + jnp.bfloat16(16 * k), one, zero)
                for k in range(2 * LOW // 16)
            ]
            columns.append(jnp.concatenate(hot, axis=0))
        picked = jnp.dot(
            plain_ref[...], jnp.concatenate(columns, axis=1), preferred_element_type=jnp.float32
        )
        for part, j in enumerate((i, i + 1)):
            want = jnp.broadcast_to(row_ref[j : j + 1, :], (8, LOW))
            value = jnp.zeros((8, LOW), jnp.float32)
            for q in range(half // 8):
                here = picked[8 * q : 8 * q + 8, part * LOW : (part + 1) * LOW]
                value = jnp.where(want == along_8 + 8 * q, here, value)
            found.append(jnp.sum(value, axis=0, keepdims=True))
        yield None
    yield jnp.concatenate(found, axis=0)


def lookup_kernel(index_ref, table_ref, scale_ref, plain_ref, out_ref, found_ref, lane_ref, row_ref):
    rows, width = index_ref.shape
    groups = rows // 8
    scale = jnp.broadcast_to(scale_ref[...], (8, LOW))
    units = COLUMNS * groups
    dotted = units // 2

    def step(t, _):
        base = pl.multiple_of(t * COLUMNS * LOW, LOW)

        def work(unit):
            column, i = unit // groups, unit % groups * 8
            index = index_ref[i : i + 8, pl.ds(base + column * LOW, LOW)]
            if unit < dotted:
                steps = by_products(index, plain_ref, lane_ref.at[unit], row_ref.at[unit])
            else:
                steps = by_gathers(index, table_ref, scale)
            for value in steps:
                if value is not None:
                    found_ref[i : i + 8, column * LOW : (column + 1) * LOW] = value
                yield

        products = [work(u) for u in range(dotted)]
        gathers = [work(u) for u in range(dotted, units)]
        first = (None for g in products for _ in g)
        second = (None for g in gathers for _ in g)
        fine = table_ref.shape[0] + 1
        for k in range((units - dotted) * fine):
            next(second, None)
            if k % (fine // 5) == 0:
                next(first, None)
        for _ in first:
            pass
        for _ in second:
            pass
        out_ref[:, pl.ds(base, COLUMNS * LOW)] = found_ref[...].astype(jnp.bfloat16)
        return 0

    lax.fori_loop(0, width // (COLUMNS * LOW), step, 0)


def lookup(index, table, scale, plain):
    groups = index.shape[0] // 8
    slots = (COLUMNS * groups // 2, 8, LOW)
    return pl.pallas_call(
        lookup_kernel,
        out_shape=out_of(index.shape, jnp.bfloat16),
        in_specs=[VMEM] * 4,
        out_specs=VMEM,
        scratch_shapes=[
            pltpu.VMEM((index.shape[0], COLUMNS * LOW), jnp.float32),
            pltpu.VMEM(slots, jnp.float32),
            pltpu.VMEM(slots, jnp.int32),
        ],
        compiler_params=room(6),
    )(index, table, scale, plain)


def ring_gather(value, first, turn, halves):
    def line(sign):
        def target(x, y, z, c):
            step = sign if c == turn else -sign
            if (c == 0) == first:
                return (x + step, y, z, c)
            return (x, y + step, z, c)

        return target

    behind = shift(value, line(1))
    ahead = shift(value, line(-1))
    if not halves:
        return [value, behind, ahead, shift(behind, line(1))]
    low = shift(half_of(behind, 0), line(1))
    high = shift(half_of(ahead, 1), line(-1))
    return [value, behind, ahead, low, high]


def half_kernel(a_ref, out_ref, *, which):
    size = out_ref.shape[0]
    out_ref[...] = a_ref[which * size : (which + 1) * size]


def half_of(a, which):
    return pl.pallas_call(
        lambda *refs: half_kernel(*refs, which=which),
        out_shape=out_of((a.shape[0] // 2, *a.shape[1:]), a.dtype),
        in_specs=[VMEM],
        out_specs=VMEM,
        compiler_params=room(3),
    )(a)


def offset(k, turn, c):
    step = jnp.where(c == turn, 1, -1)
    return (0, -step, step, 2)[k]


def stack_kernel(a0, a1, a2, a3, out_ref):
    for k, a in enumerate((a0, a1, a2, a3)):
        out_ref[k] = a[...]


def stacked(pieces):
    return pl.pallas_call(
        stack_kernel,
        out_shape=out_of((len(pieces), *pieces[0].shape), pieces[0].dtype),
        in_specs=[VMEM] * 4,
        out_specs=VMEM,
        compiler_params=room(4),
    )(*pieces)


def early_kernel(a0, a1, a2, dosage_ref, out_ref, lhs_ref):
    rows = a0.shape[0] * a0.shape[1]
    for u, a in enumerate((a0, a1, a2)):
        lhs_ref[u * rows : (u + 1) * rows, :] = a[...].reshape(rows, a.shape[2])
    out_ref[...] = jnp.dot(lhs_ref[...], dosage_ref[...], preferred_element_type=jnp.float32)


def early_product(pieces, dosage):
    rows = sum(p.shape[0] * p.shape[1] for p in pieces)
    return pl.pallas_call(
        early_kernel,
        out_shape=out_of((rows, dosage.shape[1]), jnp.float32),
        in_specs=[VMEM] * 4,
        out_specs=VMEM,
        scratch_shapes=[pltpu.VMEM((rows, dosage.shape[0]), jnp.bfloat16)],
        compiler_params=room(16),
    )(*pieces, dosage)


def late_kernel(
    early_ref, low_ref, high_ref, dosage_ref, totals_ref, keep_ref, send_ref, lhs_ref, all_ref,
    *, turn_near, turn_far,
):
    rows = low_ref.shape[1]
    half = low_ref.shape[0] * rows
    extra = keep_ref.shape[1] - 2 * rows
    dest = destinations(turn_near, turn_far)

    def place(u, t, value):
        start = pl.multiple_of(dest(u, t) * rows, rows)
        all_ref[pl.ds(start, rows), :] = value

    lhs_ref[:half, :] = low_ref[...].reshape(half, lhs_ref.shape[1])
    lhs_ref[half:, :] = high_ref[...].reshape(half, lhs_ref.shape[1])
    part = jnp.dot(lhs_ref[...], dosage_ref[...], preferred_element_type=jnp.float32)
    for u in range(RING - 1):
        for t in range(RING):
            start = (u * RING + t) * rows
            place(u, t, early_ref[start : start + rows, :])
    for t in range(RING):
        place(RING - 1, t, part[t * rows : (t + 1) * rows])
    for h, ref in enumerate((keep_ref, send_ref)):
        for k in range(RING):
            start = (h * RING + k) * 2 * rows
            ref[k, : 2 * rows, :] = all_ref[start : start + 2 * rows, :]
            if extra:
                ref[k, 2 * rows :, :] = totals_ref[...]


def late_product(early, low, high, dosage, totals, with_totals, turn_near, turn_far):
    rows = low.shape[1]
    shape = (RING, 2 * rows + (totals.shape[0] if with_totals else 0), dosage.shape[1])
    return pl.pallas_call(
        lambda *refs: late_kernel(*refs, turn_near=turn_near, turn_far=turn_far),
        out_shape=(out_of(shape, jnp.float32), out_of(shape, jnp.float32)),
        in_specs=[VMEM] * 5,
        out_specs=(VMEM, VMEM),
        scratch_shapes=[
            pltpu.VMEM((RING * rows, dosage.shape[0]), jnp.bfloat16),
            pltpu.VMEM((RING * RING * rows, dosage.shape[1]), jnp.float32),
        ],
        compiler_params=room(16),
    )(early, low, high, dosage, totals)


def add_kernel(a_ref, b_ref, o0, o1, o2, o3):
    for k, o in enumerate((o0, o1, o2, o3)):
        o[...] = a_ref[k] + b_ref[k]


def core_sum(keep, got):
    one = out_of(keep.shape[1:], jnp.float32)
    return pl.pallas_call(
        add_kernel,
        out_shape=(one,) * 4,
        in_specs=[VMEM] * 2,
        out_specs=(VMEM,) * 4,
        compiler_params=room(4),
    )(keep, got)


def destinations(turn_near, turn_far):
    x, y, z, c = (lax.axis_index(a) for a in AXES)
    step = 1 - 2 * c

    def of(u, t):
        far, near = offset(u, turn_far, c), offset(t, turn_near, c)
        px = (x + RING + jnp.where(c == 0, near, far)) % RING
        py = (y + RING + jnp.where(c == 0, far, near)) % RING
        away = jnp.where(py // 2 == c, 0, 1)
        owner = ((1 - 2 * away) * step * (px - z) + 2 * RING) % RING
        return away * 8 + owner * 2 + py % 2

    return of


def z_line(sign):
    def target(x, y, z, c):
        return (x, y, z + (sign if c == 0 else -sign), c)

    return target


def reduced(far, dosage, totals, with_totals, turn):
    early = early_product(far[:3], dosage)
    low, high = far[3:]
    keep, send = late_product(early, low, high, dosage, totals, with_totals, turn, 1)
    got = other_core(send)
    own, ahead, opposite, behind = core_sum(keep, got)
    passing = shift(opposite, z_line(1))
    from_ahead = shift(behind, z_line(-1))
    from_behind = shift(ahead + passing, z_line(1))
    return own, from_behind, from_ahead


def final_kernel(*refs, extra, count):
    if extra:
        var_ref, end_ref, p, q, r, z_ref, most_ref, inverse_ref = refs
        rows = (p.shape[0] - extra) // 2
        totals = p[2 * rows :, :] + q[2 * rows :, :] + r[2 * rows :, :]
        allele_sum = jnp.sum(totals[0:8], axis=0, keepdims=True)
        allele_sq = jnp.sum(totals[8:16], axis=0, keepdims=True)
        allele_var = allele_sq / count - (allele_sum / count) ** 2
        inverse = 1.0 / jnp.sqrt(count * (var_ref[0, 0] + EPSILON) * (allele_var + EPSILON))
        inverse_ref[...] = inverse
        places = [0, rows]
    else:
        end_ref, inverse_ref, z0, most0, p, q, r, z_ref, most_ref = refs
        rows = p.shape[0] // 2
        inverse = inverse_ref[...]
        for h in range(2):
            z_ref[2 * h * rows : (2 * h + 1) * rows, :] = z0[h * rows : (h + 1) * rows, :]
            most_ref[2 * h * rows : (2 * h + 1) * rows, :] = most0[h * rows : (h + 1) * rows, :]
        places = [rows, 3 * rows]
    width = z_ref.shape[1]
    ends = end_ref[...]
    clipped = jnp.clip(ends, 0, width - 1)
    both = 2 * rows
    z = (p[:both, :] + q[:both, :] + r[:both, :]) * inverse
    lanes = lax.broadcasted_iota(jnp.int32, (both, LOW), 1)
    lane = jnp.broadcast_to(clipped % LOW, (both, LOW))
    group = jnp.broadcast_to(clipped // LOW, (both, LOW))
    parts = [jnp.abs(z[:, g * LOW : (g + 1) * LOW]) for g in range(width // LOW)]
    wholes = [jnp.max(v, axis=1, keepdims=True) for v in parts]
    step = 1
    while step < LOW:
        parts = [
            jnp.maximum(v, jnp.where(lanes >= step, pltpu.roll(v, step, 1), 0.0)) for v in parts
        ]
        step *= 2
    chosen = jnp.zeros((both, LOW), jnp.float32)
    before = jnp.zeros((both, 1), jnp.float32)
    for g, v in enumerate(parts):
        taken = jnp.take_along_axis(v, lane, axis=1, mode="promise_in_bounds")
        chosen = jnp.where(group == g, jnp.maximum(taken, before), chosen)
        before = jnp.maximum(before, wholes[g])
    chosen = jnp.where(jnp.broadcast_to(ends >= 0, (both, LOW)), chosen, 0.0)
    for h, place in enumerate(places):
        z_ref[place : place + rows, :] = z[h * rows : (h + 1) * rows]
        most_ref[place : place + rows, :] = chosen[h * rows : (h + 1) * rows].astype(most_ref.dtype)


def final_first(pheno_var, ends, parts, extra, count):
    rows, width = parts[0].shape[0] - extra, parts[0].shape[1]
    return pl.pallas_call(
        lambda *refs: final_kernel(*refs, extra=extra, count=count),
        out_shape=(
            out_of((rows, width), jnp.float32),
            out_of((rows, ends.shape[1]), jnp.bfloat16),
            out_of((1, width), jnp.float32),
        ),
        in_specs=[SMEM] + [VMEM] * 4,
        out_specs=(VMEM,) * 3,
        compiler_params=room(4),
    )(pheno_var, ends, *parts)


def final_second(ends, inverse, z0, most0, parts, count):
    rows, width = parts[0].shape
    return pl.pallas_call(
        lambda *refs: final_kernel(*refs, extra=0, count=count),
        out_shape=(
            out_of((CHUNKS * rows, width), jnp.float32),
            out_of((CHUNKS * rows, ends.shape[1]), jnp.bfloat16),
        ),
        in_specs=[VMEM] * 7,
        out_specs=(VMEM,) * 2,
        compiler_params=room(4),
    )(ends, inverse, z0, most0, *parts)


def largest(value, first):
    def line(step):
        def target(x, y, z, c):
            return (x + step, y, z, c) if (c == 0) == first else (x, y + step, z, c)

        return target

    got = [shift(value, line(k)) for k in (2, 1, 3)]
    return jnp.maximum(jnp.maximum(value, got[0]), jnp.maximum(got[1], got[2]))


def per_device(dosage, phenotype, perm_index, seg_lengths):
    samples, width = dosage.shape
    x, y = lax.axis_index("x"), lax.axis_index("y")
    chunks = fetched(perm_index)
    dosage_bf, totals = convert_dosage(dosage)
    table, scale, pheno_var, plain = make_table(phenotype.reshape(-1, LOW))
    ends = (jnp.cumsum(seg_lengths) - 1 - (x * RING + y) * width)[None, :].astype(jnp.int32)
    count = float(samples * lax.axis_size("z") * lax.axis_size("c"))

    far = []
    for k, chunk in enumerate(chunks):
        traits = lookup(chunk, table, scale, plain)
        near = ring_gather(traits, True, k, False)
        far.append(ring_gather(stacked(near), False, 1, True))
    parts = reduced(far[0], dosage_bf, totals, True, 0)
    z0, most0, inverse = final_first(pheno_var, ends, parts, totals.shape[0], count)
    parts = reduced(far[1], dosage_bf, totals, False, 1)
    zscore, most = final_second(ends, inverse, z0, most0, parts, count)
    return (zscore, largest(largest(most, True), False).astype(jnp.float32))


def solution(mesh):
    fine = Mesh(mesh.devices.reshape(RING, RING, RING, 2), AXES)
    var, samp = ("x", "y"), ("z", "c")
    return jax.shard_map(
        per_device,
        mesh=fine,
        in_specs=(P(samp, var), P(samp), P(var, samp), P()),
        out_specs=(P(samp, var), P(samp, None)),
        check_vma=False,
    )
```

```python
import jax
import jax.numpy as jnp
from jax import lax
from jax.experimental import pallas as pl
from jax.experimental.pallas import tpu as pltpu
from jax.sharding import Mesh, PartitionSpec as P


EPSILON = 1e-05
RING = 4
AXES = ("x", "y", "z", "c")
CHUNKS = 2
LOW = 128
COLUMNS = 12
PLACES = [
    (x, y, z, c) for x in range(RING) for y in range(RING) for z in range(RING) for c in range(2)
]
VMEM = pl.BlockSpec(memory_space=pltpu.VMEM)
SMEM = pl.BlockSpec(memory_space=pltpu.SMEM)


def at(x, y, z, c):
    return (((x % RING) * RING + y % RING) * RING + z % RING) * 2 + c


def shift(value, target):
    return lax.ppermute(value, AXES, [(at(*d), at(*target(*d))) for d in PLACES])


def along(value, axis, step):
    return lax.ppermute(value, axis, [(i, (i + step) % RING) for i in range(RING)])


def other_core(value):
    return lax.ppermute(value, "c", [(0, 1), (1, 0)])


def out_of(shape, dtype):
    return jax.ShapeDtypeStruct(shape, dtype)


def room(mib):
    return pltpu.CompilerParams(vmem_limit_bytes=mib << 20)


def dosage_kernel(dosage_ref, out_ref, totals_ref, acc_ref):
    @pl.when(pl.program_id(0) == 0)
    def _():
        acc_ref[...] = jnp.zeros_like(acc_ref)

    d = dosage_ref[...]
    out_ref[...] = d.astype(jnp.bfloat16)
    groups = d.reshape(d.shape[0] // 8, 8, d.shape[1])
    acc_ref[0:8] += jnp.sum(groups, axis=0)
    acc_ref[8:16] += jnp.sum(groups * groups, axis=0)

    @pl.when(pl.program_id(0) == pl.num_programs(0) - 1)
    def _():
        totals_ref[...] = jnp.zeros_like(totals_ref)
        for k in range(2):
            total = jnp.sum(acc_ref[8 * k : 8 * k + 8, :], axis=0, keepdims=True)
            totals_ref[k : k + 1, :] = total.astype(jnp.float32)


def convert_dosage(dosage):
    samples, width = dosage.shape
    block = 512
    return pl.pallas_call(
        dosage_kernel,
        grid=(samples // block,),
        out_shape=(out_of(dosage.shape, jnp.bfloat16), out_of((8, width), jnp.float32)),
        in_specs=[pl.BlockSpec((block, width), lambda i: (i, 0))],
        out_specs=(
            pl.BlockSpec((block, width), lambda i: (i, 0)),
            pl.BlockSpec((8, width), lambda i: (0, 0)),
        ),
        scratch_shapes=[pltpu.VMEM((16, width), jnp.int32)],
        compiler_params=room(8),
    )(dosage)


def table_kernel(pair_ref, mine_ref, theirs_ref, far_ref, other_ref, *rest):
    table_ref, scale_ref, var_ref, plain_ref, code_ref, value_ref = rest
    z, c = lax.axis_index("z"), lax.axis_index("c")
    step = 1 - 2 * c
    depth = far_ref.shape[0]
    blocks = (
        (pair_ref[:depth], z, c),
        (pair_ref[depth:], z, 1 - c),
        (mine_ref[:depth], z - step, c),
        (mine_ref[depth:], z - step, 1 - c),
        (theirs_ref[:depth], z + step, 1 - c),
        (theirs_ref[depth:], z + step, c),
        (far_ref[...], z + 2, c),
        (other_ref[...], z + 2, 1 - c),
    )
    values = [b[0] for b in blocks]
    count = len(values) * values[0].size
    mean = jnp.sum(sum(values)) / count
    values = [v - mean for v in values]
    var_ref[0, 0] = jnp.sum(sum(v * v for v in values)) / count
    rounded = [v.astype(jnp.bfloat16).astype(jnp.float32) for v in values]
    most = jnp.abs(rounded[0])
    for r in rounded[1:]:
        most = jnp.maximum(most, jnp.abs(r))
    most = jnp.full((1, LOW), jnp.maximum(jnp.max(most), 1e-30), jnp.float32)
    for r, (_, at_z, core) in zip(rounded, blocks):
        code = jnp.round(jnp.sqrt(jnp.sqrt(jnp.abs(r) / most)) * 32767.0).astype(jnp.int32)
        code = jnp.where(r < 0, -code, code)
        start = pl.multiple_of((((at_z + RING) % RING) * 2 + core) * depth, 8)
        code_ref[pl.ds(start, depth), :] = code
        value_ref[pl.ds(start, depth), :] = r
    half = table_ref.shape[0]
    plain_ref[:, :LOW] = value_ref[:half, :].astype(jnp.bfloat16)
    plain_ref[:, LOW:] = value_ref[half:, :].astype(jnp.bfloat16)
    table_ref[...] = lax.shift_left(code_ref[half:, :], 16) + (code_ref[:half, :] & 0xFFFF)
    scale_ref[...] = jnp.sqrt(jnp.sqrt(most)) / 32767.0


def make_table(own):
    def line(x, y, z, c):
        return (x, y, z + 1 - 2 * c, c)

    other = other_core(own)
    far = along(own, "z", 2)
    pair = join(own, other)
    mine = shift(pair, line)
    far_other = other_core(far)
    theirs = other_core(mine)
    rows = 2 * RING * own.shape[0]
    return pl.pallas_call(
        table_kernel,
        out_shape=(
            out_of((rows // 2, LOW), jnp.int32),
            out_of((1, LOW), jnp.float32),
            out_of((1, 1), jnp.float32),
            out_of((rows // 2, 2 * LOW), jnp.bfloat16),
        ),
        in_specs=[VMEM] * 5,
        out_specs=(VMEM, VMEM, SMEM, VMEM),
        scratch_shapes=[pltpu.VMEM((rows, LOW), jnp.int32), pltpu.VMEM((rows, LOW), jnp.float32)],
        compiler_params=room(2),
    )(pair, mine, theirs, far, far_other)


def join_kernel(a_ref, b_ref, out_ref):
    out_ref[: a_ref.shape[0]] = a_ref[...]
    out_ref[a_ref.shape[0] :] = b_ref[...]


def join(a, b):
    return pl.pallas_call(
        join_kernel,
        out_shape=out_of((a.shape[0] + b.shape[0], a.shape[1]), a.dtype),
        in_specs=[VMEM] * 2,
        out_specs=VMEM,
        compiler_params=room(2),
    )(a, b)


def fetch_kernel(a_ref, *outs):
    rows = outs[0].shape[0]
    for k, out in enumerate(outs):
        out[...] = a_ref[k * rows : (k + 1) * rows, :]


def fetched(a):
    one = out_of((a.shape[0] // CHUNKS, a.shape[1]), a.dtype)
    return pl.pallas_call(
        fetch_kernel,
        out_shape=(one,) * CHUNKS,
        in_specs=[VMEM],
        out_specs=(VMEM,) * CHUNKS,
        compiler_params=room(4),
    )(a)


def places_of(index, half):
    row = lax.shift_right_logical(index, 7)
    upper = row >= half
    return index & (LOW - 1), jnp.where(upper, row - half, row), upper


def by_gathers(index, table_ref, scale):
    half = table_ref.shape[0]
    lane, row, upper = places_of(index, half)
    word = jnp.zeros((8, LOW), jnp.int32)
    for r in range(half):
        source = jnp.broadcast_to(table_ref[r : r + 1, :], (8, LOW))
        taken = jnp.take_along_axis(source, lane, axis=1, mode="promise_in_bounds")
        word = jnp.where(row == r, taken, word)
        yield None
    code = lax.shift_right_arithmetic(jnp.where(upper, word, lax.shift_left(word, 16)), 16)
    root = code.astype(jnp.float32) * scale
    root = root * root
    root = root * root
    yield jnp.where(code < 0, -root, root)


def by_products(index, plain_ref, lane_ref, row_ref):
    half = plain_ref.shape[0]
    lane, row, upper = places_of(index, half)
    lane_ref[...] = jnp.where(upper, lane + LOW, lane).astype(jnp.float32)
    row_ref[...] = row
    one = jnp.ones((16, LOW), jnp.bfloat16)
    zero = jnp.zeros((16, LOW), jnp.bfloat16)
    along_16 = lax.broadcasted_iota(jnp.int32, (16, LOW), 0).astype(jnp.float32)
    along_16 = along_16.astype(jnp.bfloat16)
    along_8 = lax.broadcasted_iota(jnp.int32, (8, LOW), 0)
    found = []
    for i in range(0, 8, 2):
        columns = []
        for j in (i, i + 1):
            want = jnp.broadcast_to(lane_ref[j : j + 1, :], (16, LOW)).astype(jnp.bfloat16)
            hot = [
                jnp.where(want == along_16 + jnp.bfloat16(16 * k), one, zero)
                for k in range(2 * LOW // 16)
            ]
            columns.append(jnp.concatenate(hot, axis=0))
        picked = jnp.dot(
            plain_ref[...], jnp.concatenate(columns, axis=1), preferred_element_type=jnp.float32
        )
        for part, j in enumerate((i, i + 1)):
            want = jnp.broadcast_to(row_ref[j : j + 1, :], (8, LOW))
            value = jnp.zeros((8, LOW), jnp.float32)
            for q in range(half // 8):
                here = picked[8 * q : 8 * q + 8, part * LOW : (part + 1) * LOW]
                value = jnp.where(want == along_8 + 8 * q, here, value)
            found.append(jnp.sum(value, axis=0, keepdims=True))
        yield None
    yield jnp.concatenate(found, axis=0)


def lookup_kernel(index_ref, table_ref, scale_ref, plain_ref, out_ref, found_ref, lane_ref, row_ref):
    rows, width = index_ref.shape
    groups = rows // 8
    scale = jnp.broadcast_to(scale_ref[...], (8, LOW))
    units = COLUMNS * groups
    dotted = units * 11 // 24

    def step(t, _):
        base = pl.multiple_of(t * COLUMNS * LOW, LOW)

        def work(unit):
            column, i = unit // groups, unit % groups * 8
            index = index_ref[i : i + 8, pl.ds(base + column * LOW, LOW)]
            if unit < dotted:
                steps = by_products(index, plain_ref, lane_ref.at[unit], row_ref.at[unit])
            else:
                steps = by_gathers(index, table_ref, scale)
            for value in steps:
                if value is not None:
                    found_ref[i : i + 8, column * LOW : (column + 1) * LOW] = value
                yield

        products = [work(u) for u in range(dotted)]
        gathers = [work(u) for u in range(dotted, units)]
        first = (None for g in products for _ in g)
        second = (None for g in gathers for _ in g)
        fine = table_ref.shape[0] + 1
        for k in range((units - dotted) * fine):
            next(second, None)
            if k % (fine // 5) == 0:
                next(first, None)
        for _ in first:
            pass
        for _ in second:
            pass
        out_ref[:, pl.ds(base, COLUMNS * LOW)] = found_ref[...].astype(jnp.bfloat16)
        return 0

    lax.fori_loop(0, width // (COLUMNS * LOW), step, 0)


def lookup(index, table, scale, plain):
    groups = index.shape[0] // 8
    slots = (COLUMNS * groups * 11 // 24, 8, LOW)
    return pl.pallas_call(
        lookup_kernel,
        out_shape=out_of(index.shape, jnp.bfloat16),
        in_specs=[VMEM] * 4,
        out_specs=VMEM,
        scratch_shapes=[
            pltpu.VMEM((index.shape[0], COLUMNS * LOW), jnp.float32),
            pltpu.VMEM(slots, jnp.float32),
            pltpu.VMEM(slots, jnp.int32),
        ],
        compiler_params=room(6),
    )(index, table, scale, plain)


def ring_gather(value, first, turn, halves):
    def line(sign):
        def target(x, y, z, c):
            step = sign if c == turn else -sign
            if (c == 0) == first:
                return (x + step, y, z, c)
            return (x, y + step, z, c)

        return target

    behind = shift(value, line(1))
    ahead = shift(value, line(-1))
    if not halves:
        return [value, behind, ahead, shift(behind, line(1))]
    low = shift(half_of(behind, 0), line(1))
    high = shift(half_of(ahead, 1), line(-1))
    return [value, behind, ahead, low, high]


def half_kernel(a_ref, out_ref, *, which):
    size = out_ref.shape[0]
    out_ref[...] = a_ref[which * size : (which + 1) * size]


def half_of(a, which):
    return pl.pallas_call(
        lambda *refs: half_kernel(*refs, which=which),
        out_shape=out_of((a.shape[0] // 2, *a.shape[1:]), a.dtype),
        in_specs=[VMEM],
        out_specs=VMEM,
        compiler_params=room(3),
    )(a)


def offset(k, turn, c):
    step = jnp.where(c == turn, 1, -1)
    return (0, -step, step, 2)[k]


def stack_kernel(a0, a1, a2, a3, out_ref):
    for k, a in enumerate((a0, a1, a2, a3)):
        out_ref[k] = a[...]


def stacked(pieces):
    return pl.pallas_call(
        stack_kernel,
        out_shape=out_of((len(pieces), *pieces[0].shape), pieces[0].dtype),
        in_specs=[VMEM] * 4,
        out_specs=VMEM,
        compiler_params=room(4),
    )(*pieces)


def early_kernel(a0, a1, a2, dosage_ref, out_ref, lhs_ref):
    rows = a0.shape[0] * a0.shape[1]
    for u, a in enumerate((a0, a1, a2)):
        lhs_ref[u * rows : (u + 1) * rows, :] = a[...].reshape(rows, a.shape[2])
    out_ref[...] = jnp.dot(lhs_ref[...], dosage_ref[...], preferred_element_type=jnp.float32)


def early_product(pieces, dosage):
    rows = sum(p.shape[0] * p.shape[1] for p in pieces)
    return pl.pallas_call(
        early_kernel,
        out_shape=out_of((rows, dosage.shape[1]), jnp.float32),
        in_specs=[VMEM] * 4,
        out_specs=VMEM,
        scratch_shapes=[pltpu.VMEM((rows, dosage.shape[0]), jnp.bfloat16)],
        compiler_params=room(16),
    )(*pieces, dosage)


def late_kernel(
    early_ref, low_ref, high_ref, dosage_ref, totals_ref, keep_ref, send_ref, lhs_ref, all_ref,
    *, turn_near, turn_far,
):
    rows = low_ref.shape[1]
    half = low_ref.shape[0] * rows
    extra = keep_ref.shape[1] - 2 * rows
    dest = destinations(turn_near, turn_far)

    def place(u, t, value):
        start = pl.multiple_of(dest(u, t) * rows, rows)
        all_ref[pl.ds(start, rows), :] = value

    lhs_ref[:half, :] = low_ref[...].reshape(half, lhs_ref.shape[1])
    lhs_ref[half:, :] = high_ref[...].reshape(half, lhs_ref.shape[1])
    part = jnp.dot(lhs_ref[...], dosage_ref[...], preferred_element_type=jnp.float32)
    for u in range(RING - 1):
        for t in range(RING):
            start = (u * RING + t) * rows
            place(u, t, early_ref[start : start + rows, :])
    for t in range(RING):
        place(RING - 1, t, part[t * rows : (t + 1) * rows])
    for h, ref in enumerate((keep_ref, send_ref)):
        for k in range(RING):
            start = (h * RING + k) * 2 * rows
            ref[k, : 2 * rows, :] = all_ref[start : start + 2 * rows, :]
            if extra:
                ref[k, 2 * rows :, :] = totals_ref[...]


def late_product(early, low, high, dosage, totals, with_totals, turn_near, turn_far):
    rows = low.shape[1]
    shape = (RING, 2 * rows + (totals.shape[0] if with_totals else 0), dosage.shape[1])
    return pl.pallas_call(
        lambda *refs: late_kernel(*refs, turn_near=turn_near, turn_far=turn_far),
        out_shape=(out_of(shape, jnp.float32), out_of(shape, jnp.float32)),
        in_specs=[VMEM] * 5,
        out_specs=(VMEM, VMEM),
        scratch_shapes=[
            pltpu.VMEM((RING * rows, dosage.shape[0]), jnp.bfloat16),
            pltpu.VMEM((RING * RING * rows, dosage.shape[1]), jnp.float32),
        ],
        compiler_params=room(16),
    )(early, low, high, dosage, totals)


def add_kernel(a_ref, b_ref, o0, o1, o2, o3):
    for k, o in enumerate((o0, o1, o2, o3)):
        o[...] = a_ref[k] + b_ref[k]


def core_sum(keep, got):
    one = out_of(keep.shape[1:], jnp.float32)
    return pl.pallas_call(
        add_kernel,
        out_shape=(one,) * 4,
        in_specs=[VMEM] * 2,
        out_specs=(VMEM,) * 4,
        compiler_params=room(4),
    )(keep, got)


def destinations(turn_near, turn_far):
    x, y, z, c = (lax.axis_index(a) for a in AXES)
    step = 1 - 2 * c

    def of(u, t):
        far, near = offset(u, turn_far, c), offset(t, turn_near, c)
        px = (x + RING + jnp.where(c == 0, near, far)) % RING
        py = (y + RING + jnp.where(c == 0, far, near)) % RING
        away = jnp.where(py // 2 == c, 0, 1)
        owner = ((1 - 2 * away) * step * (px - z) + 2 * RING) % RING
        return away * 8 + owner * 2 + py % 2

    return of


def z_line(sign):
    def target(x, y, z, c):
        return (x, y, z + (sign if c == 0 else -sign), c)

    return target


def reduced(far, dosage, totals, with_totals, turn):
    early = early_product(far[:3], dosage)
    low, high = far[3:]
    keep, send = late_product(early, low, high, dosage, totals, with_totals, turn, 1)
    got = other_core(send)
    own, ahead, opposite, behind = core_sum(keep, got)
    passing = shift(opposite, z_line(1))
    from_ahead = shift(behind, z_line(-1))
    from_behind = shift(ahead + passing, z_line(1))
    return own, from_behind, from_ahead


def final_kernel(*refs, extra, count):
    if extra:
        var_ref, end_ref, p, q, r, z_ref, most_ref, inverse_ref = refs
        rows = (p.shape[0] - extra) // 2
        totals = p[2 * rows :, :] + q[2 * rows :, :] + r[2 * rows :, :]
        allele_sum, allele_sq = totals[0:1], totals[1:2]
        allele_var = allele_sq / count - (allele_sum / count) ** 2
        inverse = 1.0 / jnp.sqrt(count * (var_ref[0, 0] + EPSILON) * (allele_var + EPSILON))
        inverse_ref[...] = inverse
        places = [0, rows]
    else:
        end_ref, inverse_ref, z0, most0, p, q, r, z_ref, most_ref = refs
        rows = p.shape[0] // 2
        inverse = inverse_ref[...]
        for h in range(2):
            z_ref[2 * h * rows : (2 * h + 1) * rows, :] = z0[h * rows : (h + 1) * rows, :]
            most_ref[2 * h * rows : (2 * h + 1) * rows, :] = most0[h * rows : (h + 1) * rows, :]
        places = [rows, 3 * rows]
    width = z_ref.shape[1]
    ends = end_ref[...]
    clipped = jnp.clip(ends, 0, width - 1)
    both = 2 * rows
    z = (p[:both, :] + q[:both, :] + r[:both, :]) * inverse
    lanes = lax.broadcasted_iota(jnp.int32, (both, LOW), 1)
    lane = jnp.broadcast_to(clipped % LOW, (both, LOW))
    group = jnp.broadcast_to(clipped // LOW, (both, LOW))
    parts = [jnp.abs(z[:, g * LOW : (g + 1) * LOW]) for g in range(width // LOW)]
    wholes = [jnp.max(v, axis=1, keepdims=True) for v in parts]
    step = 1
    while step < LOW:
        parts = [
            jnp.maximum(v, jnp.where(lanes >= step, pltpu.roll(v, step, 1), 0.0)) for v in parts
        ]
        step *= 2
    chosen = jnp.zeros((both, LOW), jnp.float32)
    before = jnp.zeros((both, 1), jnp.float32)
    for g, v in enumerate(parts):
        taken = jnp.take_along_axis(v, lane, axis=1, mode="promise_in_bounds")
        chosen = jnp.where(group == g, jnp.maximum(taken, before), chosen)
        before = jnp.maximum(before, wholes[g])
    chosen = jnp.where(jnp.broadcast_to(ends >= 0, (both, LOW)), chosen, 0.0)
    for h, place in enumerate(places):
        z_ref[place : place + rows, :] = z[h * rows : (h + 1) * rows]
        most_ref[place : place + rows, :] = chosen[h * rows : (h + 1) * rows].astype(most_ref.dtype)


def final_first(pheno_var, ends, parts, extra, count):
    rows, width = parts[0].shape[0] - extra, parts[0].shape[1]
    return pl.pallas_call(
        lambda *refs: final_kernel(*refs, extra=extra, count=count),
        out_shape=(
            out_of((rows, width), jnp.float32),
            out_of((rows, ends.shape[1]), jnp.bfloat16),
            out_of((1, width), jnp.float32),
        ),
        in_specs=[SMEM] + [VMEM] * 4,
        out_specs=(VMEM,) * 3,
        compiler_params=room(4),
    )(pheno_var, ends, *parts)


def final_second(ends, inverse, z0, most0, parts, count):
    rows, width = parts[0].shape
    return pl.pallas_call(
        lambda *refs: final_kernel(*refs, extra=0, count=count),
        out_shape=(
            out_of((CHUNKS * rows, width), jnp.float32),
            out_of((CHUNKS * rows, ends.shape[1]), jnp.bfloat16),
        ),
        in_specs=[VMEM] * 7,
        out_specs=(VMEM,) * 2,
        compiler_params=room(4),
    )(ends, inverse, z0, most0, *parts)


def largest(value, first):
    def line(step):
        def target(x, y, z, c):
            return (x + step, y, z, c) if (c == 0) == first else (x, y + step, z, c)

        return target

    got = [shift(value, line(k)) for k in (2, 1, 3)]
    return jnp.maximum(jnp.maximum(value, got[0]), jnp.maximum(got[1], got[2]))


def per_device(dosage, phenotype, perm_index, seg_lengths):
    samples, width = dosage.shape
    x, y = lax.axis_index("x"), lax.axis_index("y")
    chunks = fetched(perm_index)
    dosage_bf, totals = convert_dosage(dosage)
    table, scale, pheno_var, plain = make_table(phenotype.reshape(-1, LOW))
    ends = (jnp.cumsum(seg_lengths) - 1 - (x * RING + y) * width)[None, :].astype(jnp.int32)
    count = float(samples * lax.axis_size("z") * lax.axis_size("c"))

    far = []
    for k, chunk in enumerate(chunks):
        traits = lookup(chunk, table, scale, plain)
        near = ring_gather(traits, True, k, False)
        far.append(ring_gather(stacked(near), False, 1, True))
    parts = reduced(far[0], dosage_bf, totals, True, 0)
    z0, most0, inverse = final_first(pheno_var, ends, parts, totals.shape[0], count)
    parts = reduced(far[1], dosage_bf, totals, False, 1)
    zscore, most = final_second(ends, inverse, z0, most0, parts, count)
    return (zscore, largest(largest(most, True), False).astype(jnp.float32))


def solution(mesh):
    fine = Mesh(mesh.devices.reshape(RING, RING, RING, 2), AXES)
    var, samp = ("x", "y"), ("z", "c")
    return jax.shard_map(
        per_device,
        mesh=fine,
        in_specs=(P(samp, var), P(samp), P(var, samp), P()),
        out_specs=(P(samp, var), P(samp, None)),
        check_vma=False,
    )
```
